256 devices in a mesh: shift: 4 (over y_lo, core), band: 4 (over z_lo), lane: 16 (over z_hi, y_hi, x).
Axes of the slice: x: 4, y: 4 (y_hi: 2, y_lo: 2; y = y_hi * 2 + y_lo), z: 8 (z_hi: 2, z_lo: 4; z = z_hi * 4 + z_lo), core: 2. Of those that a mesh axis runs over, the one named last changes fastest.
Arguments:
- source_terms: float32 [1024, 1024, 128], P(('shift', 'band'), 'lane'), parts along dimension 0, may hold values from -6 to 6
- initial_values: float32 [1024, 1024, 128], P(('shift', 'band'), 'lane'), parts along dimension 0, may hold values from -6 to 6
- absorption: float32 [1024, 1024, 128], P(('shift', 'band'), 'lane'), parts along dimension 0, may hold values from 0.1 to 0.9
Outputs:
- corrected: float32 [1024, 1024, 128], P(('shift', 'band'), 'lane'), parts along dimension 0
The draws below stay inside these ranges and needn't reach their ends.
There are 4 independent parts, one for each index of `shift`. The reference program is written for one: setup_inputs(seed, part) draws one part's arguments, and reference() takes and returns one part's arrays. A program takes and returns all parts, laid end to end along the dimension named above; each array names one. Nothing has to cross between parts.
All inputs are finite; a program needn't handle non-finite values.
Results may differ from the reference program's by a relative error of at most 0.0003.
Values sent between devices are 32-bit elements.
A program may use at most 64 MiB of HBM per device.

```python
import jax
import jax.numpy as jnp
from jax import lax

CASES = 128
RATIO = 2
BEFORE = 3
AFTER = 3
INNER = 13
GRID_Y = 256
GRID_X = 1024


def level_of(key, extent, pieces, low, largest):
    loudness, own = 1.0, jax.random.fold_in(key, 6)
    for axis_at, shards_of in pieces:
        heights = jnp.exp(jax.random.uniform(jax.random.fold_in(own, axis_at), (shards_of,), jnp.float32, low / len(pieces), largest / len(pieces)))
        loudness = loudness * jnp.repeat(heights, extent[axis_at] // shards_of).reshape([-1 if axis == axis_at else 1 for axis in range(len(extent))])
    return loudness


def noise(stream_key, extent, spread, bound, split=(), held_as=jnp.bfloat16):
    drawn = spread * jax.random.normal(stream_key, extent, jnp.float32)
    if split:
        drawn = drawn * level_of(stream_key, extent, split, -0.22, 0.18)
    return jnp.clip(drawn, -bound, bound).astype(held_as)


def setup_inputs(seed: int = 0, part: int = 0) -> dict:
    arg_keys = jax.random.split(jax.random.key(seed), 4)
    part_keys = jax.random.split(jax.random.fold_in(arg_keys[3], part), 4)
    source_terms = noise(part_keys[0], (GRID_Y, GRID_X, CASES), 1.0, 6.0, ((0, 4), (1, 16)), jnp.float32)
    initial_values = noise(part_keys[1], (GRID_Y, GRID_X, CASES), 1.0, 6.0, ((0, 4), (1, 16)), jnp.float32)
    absorption = jnp.clip(0.1 + 0.79999997 * jax.random.uniform(part_keys[2], (GRID_Y, GRID_X, CASES), jnp.float32) ** level_of(part_keys[2], (GRID_Y, GRID_X, CASES), ((0, 4), (1, 16)), -0.2, 0.2), 0.1, 0.9)
    return {"source_terms": source_terms, "initial_values": initial_values, "absorption": absorption}


def neighbour_sum(padded):
    inner_y, inner_x = padded.shape[0] - 2, padded.shape[1] - 2
    middle_rows = lax.slice_in_dim(padded, 1, 1 + inner_y, axis=0)
    middle_columns = lax.slice_in_dim(padded, 1, 1 + inner_x, axis=1)
    return (lax.slice_in_dim(middle_columns, 0, inner_y, axis=0) + lax.slice_in_dim(middle_columns, 2, 2 + inner_y, axis=0)
            + lax.slice_in_dim(middle_rows, 0, inner_x, axis=1) + lax.slice_in_dim(middle_rows, 2, 2 + inner_x, axis=1))


def sweep_once(padded, values, load, mass_here):
    return values + 0.8 * (load + neighbour_sum(padded) - (4.0 + mass_here) * values) / (4.0 + mass_here)


def block_means(values):
    cut = values.reshape(values.shape[0] // RATIO, RATIO, values.shape[1] // RATIO, RATIO, values.shape[2])
    return jnp.mean(cut, axis=(1, 3))


def spread_blocks(values):
    return jnp.repeat(jnp.repeat(values, RATIO, axis=0), RATIO, axis=1)


def reference(source_terms, initial_values, absorption):
    values = initial_values
    for sweep in range(BEFORE):
        values = sweep_once(jnp.pad(values, ((1, 1), (1, 1), (0, 0)), mode="constant"), values, source_terms, absorption)
    defect = source_terms + neighbour_sum(jnp.pad(values, ((1, 1), (1, 1), (0, 0)), mode="constant")) - (4.0 + absorption) * values
    coarse_load, coarse_mass = block_means(defect) * RATIO, block_means(absorption) * RATIO
    coarse_values = jnp.zeros_like(coarse_load)
    for sweep in range(INNER):
        coarse_values = sweep_once(jnp.pad(coarse_values, ((1, 1), (1, 1), (0, 0)), mode="constant"), coarse_values, coarse_load, coarse_mass)
    values = values + spread_blocks(coarse_values)
    for sweep in range(AFTER):
        values = sweep_once(jnp.pad(values, ((1, 1), (1, 1), (0, 0)), mode="constant"), values, source_terms, absorption)
    corrected = values
    return corrected
```

```python
import functools

import jax
import jax.numpy as jnp
from jax import lax
from jax.experimental import pallas as pl
from jax.experimental.pallas import tpu as pltpu
from jax.sharding import PartitionSpec as P

RATIO = 2
INNER = 13
SUB = 8
BLOCK = 4
MESH = pl.DeviceIdType.MESH
DIRS = [(-1, 0), (1, 0), (0, -1), (0, 1), (-1, -1), (-1, 1), (1, -1), (1, 1)]
TOP = 4
CTOP = 16
LEVELS = 14
PITCH = 88
MARGIN = 8


class Grid:
    def __init__(self, columns, pieces, halo):
        self.columns, self.pieces, self.halo = columns, pieces, halo
        self.width = pieces * SUB
        self.stored = columns + 2 * halo

    def at(self, column, piece=0):
        return pl.multiple_of((column + self.halo) * self.width + piece * SUB, SUB)

    def boxes(self, ref):
        return ref.reshape(self.stored, self.pieces, SUB, 128)


def kernel(fine, coarse, src_hbm, init_hbm, abs_hbm, out_ref, *scratch):
    u, v, x, w, f, y, iw, ra, rs, cw, cf, ca, cb, out, sums, in_sem, send_sem, recv_sem = scratch
    band, lane = lax.axis_index("band"), lax.axis_index("lane")
    bands, lanes = lax.axis_size("band"), lax.axis_size("lane")
    rows = fine.columns
    right = lane < lanes // 2

    def exists(q):
        dy, dx = q
        there = None
        if dy:
            there = (band > 0) if dy < 0 else (band < bands - 1)
        if dx:
            beside = (lane > 0) if dx < 0 else (lane < lanes - 1)
            there = beside if not dy else there & beside
        return there

    def name_of(q):
        return {"band": band + q[0], "lane": lane + q[1]}

    def late(q):
        return right if q[1] > 0 else jnp.logical_not(right)

    def side(if_right, if_left):
        return jnp.where(right, if_right, if_left)

    barrier = pltpu.get_barrier_semaphore()
    for q in DIRS:
        @pl.when(exists(q))
        def _():
            pl.semaphore_signal(barrier, inc=1, device_id=name_of(q), device_id_type=MESH)

    inputs = ((abs_hbm, ra), (src_hbm, rs), (init_hbm, u))
    for i, (ref, held) in enumerate(inputs):
        @pl.loop(0, rows)
        def _(row):
            at = row + TOP
            place = (at % fine.pieces) * SUB + at // fine.pieces
            to = held.reshape(fine.stored, fine.width, 128).at[
                pl.ds(fine.halo, fine.columns), pl.ds(place, 1), :
            ]
            pltpu.make_async_copy(ref.at[row].reshape(fine.columns, 1, 128), to, in_sem.at[i]).start()

    def loaded(i):
        ref, held = inputs[i]
        whole = held.reshape(fine.stored, fine.width, 128).at[pl.ds(fine.halo, fine.columns), pl.ds(0, rows), :]
        pltpu.make_async_copy(ref, whole, in_sem.at[i]).wait()

    zero = jnp.zeros((SUB, 128), jnp.float32)
    for dx in (-1, 1):
        @pl.when(jnp.logical_not(exists((0, dx))))
        def _():
            for g, refs, depth in ((fine, (u, w, f, y), 4), (coarse, (cw, cf), LEVELS)):
                @pl.loop(0, depth)
                def _(j):
                    column = j - depth if dx < 0 else g.columns + j
                    for ref in refs:
                        for p in range(g.pieces):
                            ref[pl.ds(g.at(column, p), SUB), :] = zero

    for dy in (-1, 1):
        @pl.when(jnp.logical_not(exists((dy, 0))))
        def _():
            @pl.loop(0, fine.stored // SUB)
            def _(j):
                for ref in (u, w, f, y):
                    for p in range(TOP):
                        place = p * SUB if dy < 0 else (fine.pieces - 1 - p) * SUB + SUB - 1
                        ref[pl.ds(j * SUB * fine.width + place, SUB, stride=fine.width), :] = zero

            @pl.loop(0, coarse.stored)
            def _(j):
                for ref in (cw, cf):
                    for p in range(coarse.pieces):
                        at = coarse.width * j + p * SUB + (0 if dy < 0 else SUB - 2)
                        ref[pl.ds(at, 2), :] = zero[:2]

    def columns_of(g, dx, depth, skip=0):
        if dx > 0:
            return g.halo + g.columns - depth - skip, g.halo - depth - skip, depth
        return g.halo + skip, g.halo + g.columns + skip, depth

    def fine_rows(dy, depth):
        if dy > 0:
            return (5 - depth, 7), (4 - depth, 0), (depth, 1)
        return (4, 0), (5, 7), (depth, 1)

    def coarse_rows(dy, depth):
        d = depth // SUB
        if dy > 0:
            return (0, 6 - d), (0, 2 - d), (SUB, d)
        return (0, 2), (0, 6), (SUB, d)

    own = [((0, 1), (0, 1), (4, 7)), ((4, 0), (4, 0), (1, 8)), ((5, 0), (5, 0), (4, 7))]
    middle = [((0, 2), (0, 2), (SUB, 4))]

    copies = {}
    counter = [0]

    def add(name, g, source, target, q, columns, places):
        from_column, to_column, count = columns
        for (p, s), (pt, st), (np_, ns) in places:
            here = g.boxes(source).at[pl.ds(from_column, count), pl.ds(p, np_), pl.ds(s, ns), :]
            there = g.boxes(target).at[pl.ds(to_column, count), pl.ds(pt, np_), pl.ds(st, ns), :]
            copies.setdefault((name, q), []).append((here, there))

    def fine_set(name, source, target, depth, corner):
        for q in DIRS:
            dy, dx = q
            if not dy:
                add(name, fine, source, target, q, columns_of(fine, dx, depth), own)
            elif not dx:
                add(name, fine, source, target, q, (fine.halo, fine.halo, fine.columns), [fine_rows(dy, depth)])
            else:
                add(name, fine, source, target, q, columns_of(fine, dx, corner), [fine_rows(dy, corner)])

    fine_set("u", u, u, 4, 3)
    fine_set("w", w, w, 3, 2)
    fine_set("f", f, f, 3, 2)
    fine_set("y", v, y, 3, 2)
    for q in DIRS:
        dy, dx = q
        if not dy:
            add("cw", coarse, cw, cw, q, columns_of(coarse, dx, LEVELS - 1), middle)
            add("near", coarse, cf, cf, q, columns_of(coarse, dx, 2), middle)
            add("far", coarse, cf, cf, q, columns_of(coarse, dx, LEVELS - 2, 2), middle)
        elif not dx:
            place = [coarse_rows(dy, 16)]
            add("cw", coarse, cw, cw, q, (coarse.halo, coarse.halo, coarse.columns), place)
            at = coarse.halo + side(coarse.columns - 2, 0)
            add("near", coarse, cf, cf, q, (at, at, 2), place)
            at = coarse.halo + side(0, 2)
            add("far", coarse, cf, cf, q, (at, at, coarse.columns - 2), place)
        else:
            add("cw", coarse, cw, cw, q, columns_of(coarse, dx, 5), [coarse_rows(dy, 16)])
            add("cw", coarse, cw, cw, q, columns_of(coarse, dx, 7, 5), [coarse_rows(dy, 8)])
            add("near", coarse, cf, cf, q, columns_of(coarse, dx, 2), [coarse_rows(dy, 16)])
            add("far", coarse, cf, cf, q, columns_of(coarse, dx, 3, 2), [coarse_rows(dy, 16)])
            add("far", coarse, cf, cf, q, columns_of(coarse, dx, 8, 5), [coarse_rows(dy, 8)])

    first = {}
    for key in sorted(copies, key=lambda k: (k[0], DIRS.index(k[1]))):
        first[key] = counter[0]
        counter[0] += len(copies[key])

    def copies_of(name, q, arriving):
        back = (-q[0], -q[1])
        sent = copies[name, back if arriving else q]
        for i, (here, there) in enumerate(sent):
            yield pltpu.make_async_remote_copy(
                src_ref=here,
                dst_ref=there,
                send_sem=send_sem.at[first[name, q] + i],
                recv_sem=recv_sem.at[first[name, q if arriving else back] + i],
                device_id=name_of(q),
                device_id_type=MESH,
            )

    def start(name, q, when=None):
        @pl.when(exists(q) if when is None else exists(q) & when)
        def _():
            for copy in copies_of(name, q, False):
                copy.start()

    def sent(names):
        for name in names:
            for q in DIRS:
                @pl.when(exists(q))
                def _():
                    for copy in copies_of(name, q, False):
                        copy.wait_send()

    def arrived(names, q, when=None):
        @pl.when(exists(q) if when is None else exists(q) & when)
        def _():
            for name in names:
                for copy in copies_of(name, q, True):
                    copy.wait_recv()

    rows_only, sides, corners = DIRS[:2], DIRS[2:4], DIRS[4:]

    def early_arrived(names):
        for q in rows_only:
            arrived(names, q)
        for q in sides + corners:
            arrived(names, q, jnp.logical_not(late(q)))

    def late_arrived(names):
        for q in sides + corners:
            arrived(names, q, late(q))

    def get(g, ref, column, p):
        return ref[pl.ds(g.at(column, p), SUB), :]

    def stencil(g, old, column, p, count):
        here = [get(g, old, column + j, p) for j in range(-1, count + 1)]
        found = []
        for j in range(count):
            up = get(g, old, column + j, p - 1) if p else pltpu.roll(get(g, old, column + j, g.pieces - 1), 1, 0)
            if p < g.pieces - 1:
                down = get(g, old, column + j, p + 1)
            else:
                down = pltpu.roll(get(g, old, column + j, 0), SUB - 1, 0)
            found.append((here[j + 1], (up + down) + (here[j] + here[j + 2])))
        return found

    def sweep(g, old, new, weight, load, at, blocks):
        @pl.loop(0, blocks)
        def _(b):
            column = at + BLOCK * b
            for p in range(g.pieces):
                for j, (here, total) in enumerate(stencil(g, old, column, p, BLOCK)):
                    c = column + j
                    value = 0.2 * here + get(g, load, c, p) + get(g, weight, c, p) * total
                    if new is out:
                        new[pl.ds(p * PITCH + c + MARGIN, SUB, stride=g.pieces * PITCH), :] = value
                    else:
                        new[pl.ds(g.at(c, p), SUB), :] = value

    def natural(ref, column, i):
        return ref[pl.ds((column + coarse.halo) * coarse.width + 2 + i, SUB, stride=coarse.pieces), :]

    def put_natural(ref, column, i, value):
        ref[pl.ds((column + coarse.halo) * coarse.width + 2 + i, SUB, stride=coarse.pieces), :] = value

    def paired(slot, i):
        at = slot * 96 + 16 * i + TOP
        return sums[pl.ds(at, SUB, stride=2), :] + sums[pl.ds(at + 1, SUB, stride=2), :]

    def restrict(at, blocks):
        @pl.loop(0, blocks)
        def _(b):
            column = at + RATIO * b
            for p in range(fine.pieces):
                found = stencil(fine, v, RATIO * column, p, BLOCK)
                defects = []
                for j, (here, total) in enumerate(found):
                    c = RATIO * column + j
                    change = get(fine, f, c, p) + get(fine, w, c, p) * total - 0.8 * here
                    defects.append(change * get(fine, iw, c, p))
                for slot in range(2):
                    sums[pl.ds(slot * 96 + p, SUB, stride=fine.pieces), :] = defects[2 * slot] + defects[2 * slot + 1]
            for slot in range(2):
                for i in range(4):
                    put_natural(
                        cf, column + slot, i, (paired(slot, i) * (1.0 / RATIO)) * natural(cw, column + slot, i)
                    )

    def correct(values, at, blocks):
        @pl.loop(0, blocks)
        def _(b):
            column = at + RATIO * b
            for slot in range(2):
                for i in range(-1, 5):
                    more = natural(values, column + slot, i)
                    place = slot * 96 + 16 * (i + 1)
                    sums[pl.ds(place, SUB, stride=2), :] = more
                    sums[pl.ds(place + 1, SUB, stride=2), :] = more
            for slot in range(2):
                for p in range(fine.pieces):
                    more = sums[pl.ds(slot * 96 + CTOP - TOP + p, SUB, stride=fine.pieces), :]
                    for j in range(RATIO):
                        c = fine.at(RATIO * (column + slot) + j, p)
                        v[pl.ds(c, SUB), :] = v[pl.ds(c, SUB), :] + more

    loaded(0)
    loaded(1)

    @pl.loop(0, fine.columns)
    def _(c):
        for p in range(fine.pieces):
            s, n = (1, 7) if p < 4 else (0, 8) if p == 4 else (0, 7)
            at = (c + fine.halo) * fine.width + p * SUB + s
            g4 = 4.0 + ra[pl.ds(at, n), :]
            weight = 0.8 / g4
            w[pl.ds(at, n), :] = weight
            f[pl.ds(at, n), :] = weight * rs[pl.ds(at, n), :]
            iw[pl.ds(at, n), :] = 1.25 * g4

    @pl.loop(0, coarse.columns // 2)
    def _(b):
        for slot in range(2):
            c = RATIO * (2 * b + slot)
            for p in range(fine.pieces):
                total = (4.0 + get(fine, ra, c, p)) + (4.0 + get(fine, ra, c + 1, p))
                sums[pl.ds(slot * 96 + p, SUB, stride=fine.pieces), :] = total
        for slot in range(2):
            for i in range(4):
                mean = paired(slot, i) * (1.0 / RATIO) - (4.0 * RATIO - 4.0)
                put_natural(cw, 2 * b + slot, i, 0.8 / mean)

    loaded(2)
    on_band = (band > 0).astype(jnp.int32) + (band < bands - 1).astype(jnp.int32)
    on_lane = (lane > 0).astype(jnp.int32) + (lane < lanes - 1).astype(jnp.int32)
    pl.semaphore_wait(barrier, (on_band + 1) * (on_lane + 1) - 1)

    for name in ("u", "w", "f"):
        for q in sides:
            start(name, q)
    for name in ("u", "w", "f"):
        for q in corners:
            start(name, q)
    for name in ("u", "w", "f"):
        for q in rows_only:
            start(name, q)
    for q in sides + corners + rows_only:
        start("cw", q)

    before = ((u, v), (v, x), (x, v))
    early_arrived(("u", "w", "f"))
    for k, (old, new) in enumerate(before, 1):
        width = 4 * -(-(68 - 2 * k) // 4)
        sweep(fine, old, new, w, f, side(64 - k - width, k), width // 4)
    restrict(side(0, 2), 15)
    for q in sides + corners:
        start("far", q)
    for q in sides + corners:
        start("near", q, jnp.logical_not(late(q)))
    for q in rows_only:
        start("far", q)
    late_arrived(("u", "w", "f"))
    for k, (old, new) in enumerate(before, 1):
        sweep(fine, old, new, w, f, side(64 - k, k - 4), 1)
    restrict(side(30, 0), 1)
    for q in sides + corners:
        start("near", q, late(q))
    for q in rows_only:
        start("near", q)
    for q in sides + corners + rows_only:
        start("y", q)

    inner = []
    old = cf
    for k in range(2, INNER + 1):
        new = ca if k % 2 == 0 else cb
        inner.append((k, old, new))
        old = new
    sent(("u", "w", "f", "cw"))
    early_arrived(("cw", "far", "near"))
    for k, old, new in inner:
        width = 4 * -(-(48 - 2 * k) // 4)
        sweep(coarse, old, new, cw, cf, side(33 - k - width, k - 1), width // 4)

    last = inner[-1][2]
    after = ((v, u), (u, v), (v, out))

    def take(column):
        @pl.loop(0, 3)
        def _(j):
            for p in range(fine.pieces):
                at = fine.at(column + j, p)
                v[pl.ds(at, SUB), :] = y[pl.ds(at, SUB), :]

    def deliver(at):
        @pl.loop(0, rows)
        def _(row):
            for i in range(4):
                c = pl.multiple_of(at + SUB * i, SUB)
                place = pl.multiple_of((row + TOP) * PITCH + MARGIN + c, SUB)
                out_ref[row, pl.ds(c, SUB), :] = out[pl.ds(place, SUB), :]

    sent(("y", "far", "near"))
    early_arrived(("y",))

    @pl.loop(0, fine.columns // SUB)
    def _(j):
        for p, s in ((1, 0), (2, 0), (3, 0), (5, 7), (6, 7), (7, 7)):
            at = (j * SUB + fine.halo) * fine.width + p * SUB + s
            v[pl.ds(at, SUB, stride=fine.width), :] = y[pl.ds(at, SUB, stride=fine.width), :]

    take(side(-3, 64))
    correct(last, side(-2, 12), 11)
    for m, (old, new) in enumerate(after, 1):
        width = 4 * -(-(43 - 2 * m) // 4)
        sweep(fine, old, new, w, f, side(40 - m - width, 24 + m), width // 4)
    deliver(side(0, 32))

    late_arrived(("cw", "far", "near"))
    for k, old, new in inner:
        sweep(coarse, old, new, cw, cf, side(33 - k, k - 17), 4)
    late_arrived(("y",))
    take(side(64, -3))
    correct(last, side(20, -2), 7)
    for m, (old, new) in enumerate(after, 1):
        sweep(fine, old, new, w, f, side(40 - m, m - 4), 7)
    deliver(side(32, 0))


def per_device(source_terms, initial_values, absorption):
    rows, columns, cases = source_terms.shape
    fine = Grid(columns, (rows + 2 * TOP) // SUB, 8)
    coarse = Grid(columns // RATIO, (rows // RATIO + 2 * CTOP) // SUB, 18)

    def held(*shape):
        return pltpu.VMEM(shape + (cases,), jnp.float32)

    shapes = [held(fine.stored * fine.width) for _ in range(9)]
    shapes += [held(coarse.stored * coarse.width) for _ in range(4)]
    shapes += [held((rows + 2 * TOP) * PITCH), held(2 * 96)]
    count = 128
    shapes += [
        pltpu.SemaphoreType.DMA((3,)),
        pltpu.SemaphoreType.DMA((count,)),
        pltpu.SemaphoreType.DMA((count,)),
    ]
    return pl.pallas_call(
        functools.partial(kernel, fine, coarse),
        out_shape=jax.ShapeDtypeStruct(source_terms.shape, jnp.float32),
        in_specs=[pl.BlockSpec(memory_space=pltpu.HBM)] * 3,
        out_specs=pl.BlockSpec(memory_space=pltpu.VMEM),
        scratch_shapes=shapes,
        compiler_params=pltpu.CompilerParams(
            collective_id=0, has_side_effects=True, vmem_limit_bytes=52 * 1024 * 1024
        ),
    )(*[pltpu.with_memory_space_constraint(x, pltpu.HBM) for x in (source_terms, initial_values, absorption)])


def solution(mesh):
    placed = P(("shift", "band"), "lane", None)
    return jax.shard_map(
        per_device,
        mesh=mesh,
        in_specs=(placed, placed, placed),
        out_specs=placed,
        check_vma=False,
    )
```

```python
import functools

import jax
import jax.numpy as jnp
from jax import lax
from jax.experimental import pallas as pl
from jax.experimental.pallas import tpu as pltpu
from jax.sharding import PartitionSpec as P

RATIO = 2
INNER = 13
SUB = 8
BLOCK = 4
MESH = pl.DeviceIdType.MESH
DIRS = [(-1, 0), (1, 0), (0, -1), (0, 1), (-1, -1), (-1, 1), (1, -1), (1, 1)]
TOP = 4
CTOP = 16
LEVELS = 14
PITCH = 88
MARGIN = 8


class Grid:
    def __init__(self, columns, pieces, halo):
        self.columns, self.pieces, self.halo = columns, pieces, halo
        self.width = pieces * SUB
        self.stored = columns + 2 * halo

    def at(self, column, piece=0):
        return pl.multiple_of((column + self.halo) * self.width + piece * SUB, SUB)

    def boxes(self, ref):
        return ref.reshape(self.stored, self.pieces, SUB, 128)


def kernel(fine, coarse, src_hbm, init_hbm, abs_hbm, out_ref, *scratch):
    u, v, x, w, f, y, iw, ra, rs, cw, cf, ca, cb, out, sums, fine_relay, coarse_relay, in_sem, send_sem, recv_sem, pass_sem, land_sem = scratch
    band, lane = lax.axis_index("band"), lax.axis_index("lane")
    bands, lanes = lax.axis_size("band"), lax.axis_size("lane")
    rows = fine.columns
    right = lane < lanes // 2

    def exists(q):
        dy, dx = q
        there = None
        if dy:
            there = (band > 0) if dy < 0 else (band < bands - 1)
        if dx:
            beside = (lane > 0) if dx < 0 else (lane < lanes - 1)
            there = beside if not dy else there & beside
        return there

    def name_of(q):
        return {"band": band + q[0], "lane": lane + q[1]}

    def late(q):
        return right if q[1] > 0 else jnp.logical_not(right)

    def side(if_right, if_left):
        return jnp.where(right, if_right, if_left)

    low, high = lanes // 2 - 1, lanes // 2
    ends = {(0, 1): (low, high), (0, -1): (high, low)}
    relays = {
        (0, 1): {1: lanes // 4 - 1, 2: 0},
        (0, -1): {1: lanes - lanes // 4, 2: lanes - 1},
    }
    legs = []
    for q, (source, target) in ends.items():
        for relay in relays[q].values():
            legs += [(source, relay), (relay, source), (relay, target), (target, relay)]

    barrier = pltpu.get_barrier_semaphore()
    for q in DIRS:
        @pl.when(exists(q))
        def _():
            pl.semaphore_signal(barrier, inc=1, device_id=name_of(q), device_id_type=MESH)
    for source, target in legs:
        @pl.when(lane == source)
        def _():
            pl.semaphore_signal(barrier, inc=1, device_id={"lane": target}, device_id_type=MESH)

    inputs = ((abs_hbm, ra), (src_hbm, rs), (init_hbm, u))
    for i, (ref, held) in enumerate(inputs):
        @pl.loop(0, rows)
        def _(row):
            at = row + TOP
            place = (at % fine.pieces) * SUB + at // fine.pieces
            to = held.reshape(fine.stored, fine.width, 128).at[
                pl.ds(fine.halo, fine.columns), pl.ds(place, 1), :
            ]
            pltpu.make_async_copy(ref.at[row].reshape(fine.columns, 1, 128), to, in_sem.at[i]).start()

    def loaded(i):
        ref, held = inputs[i]
        whole = held.reshape(fine.stored, fine.width, 128).at[pl.ds(fine.halo, fine.columns), pl.ds(0, rows), :]
        pltpu.make_async_copy(ref, whole, in_sem.at[i]).wait()

    zero = jnp.zeros((SUB, 128), jnp.float32)
    for dx in (-1, 1):
        @pl.when(jnp.logical_not(exists((0, dx))))
        def _():
            for g, refs, depth in ((fine, (u, w, f, y), 4), (coarse, (cw, cf), LEVELS)):
                @pl.loop(0, depth)
                def _(j):
                    column = j - depth if dx < 0 else g.columns + j
                    for ref in refs:
                        for p in range(g.pieces):
                            ref[pl.ds(g.at(column, p), SUB), :] = zero

    for dy in (-1, 1):
        @pl.when(jnp.logical_not(exists((dy, 0))))
        def _():
            @pl.loop(0, fine.stored // SUB)
            def _(j):
                for ref in (u, w, f, y):
                    for p in range(TOP):
                        place = p * SUB if dy < 0 else (fine.pieces - 1 - p) * SUB + SUB - 1
                        ref[pl.ds(j * SUB * fine.width + place, SUB, stride=fine.width), :] = zero

            @pl.loop(0, coarse.stored)
            def _(j):
                for ref in (cw, cf):
                    for p in range(coarse.pieces):
                        at = coarse.width * j + p * SUB + (0 if dy < 0 else SUB - 2)
                        ref[pl.ds(at, 2), :] = zero[:2]

    def columns_of(g, dx, depth, skip=0):
        if dx > 0:
            return g.halo + g.columns - depth - skip, g.halo - depth - skip, depth
        return g.halo + skip, g.halo + g.columns + skip, depth

    def fine_rows(dy, depth):
        if dy > 0:
            return (5 - depth, 7), (4 - depth, 0), (depth, 1)
        return (4, 0), (5, 7), (depth, 1)

    def coarse_rows(dy, depth):
        e = depth - SUB
        if e <= 0:
            if dy > 0:
                return [((SUB - depth, 5), (SUB - depth, 1), (depth, 1))]
            return [((0, 2), (0, 6), (depth, 1))]
        if dy > 0:
            return [((SUB - e, 4), (SUB - e, 0), (e, 2)), ((0, 5), (0, 1), (SUB - e, 1))]
        return [((0, 2), (0, 6), (e, 2)), ((e, 2), (e, 6), (SUB - e, 1))]

    own = [((0, 1), (0, 1), (4, 7)), ((4, 0), (4, 0), (1, 8)), ((5, 0), (5, 0), (4, 7))]
    middle = [((0, 2), (0, 2), (SUB, 4))]

    copies, used = {}, {}
    offsets = {"w": 0, "f": 0, "y": 9, "cw": 0, "far": 4}
    counter = [0]

    def add(name, g, source, target, q, columns, places, paths=(0,)):
        from_column, to_column, count = columns
        for i, ((p, s), (pt, st), (np_, ns)) in enumerate(places):
            here = g.boxes(source).at[pl.ds(from_column, count), pl.ds(p, np_), pl.ds(s, ns), :]
            there = g.boxes(target).at[pl.ds(to_column, count), pl.ds(pt, np_), pl.ds(st, ns), :]
            path = paths[i % len(paths)]
            relay = None
            if path:
                held = fine_relay if g is fine else coarse_relay
                base = used.setdefault((name, q, path), 0)
                used[name, q, path] = base + count
                base += offsets[name]
                relay = held.reshape(held.shape[0] // g.width, g.pieces, SUB, 128).at[
                    pl.ds(base, count), pl.ds(p, np_), pl.ds(s, ns), :
                ]
            copies.setdefault((name, q), []).append((here, there, path, relay))

    def fine_set(name, source, target, depth, corner, paths=(0,)):
        for q in DIRS:
            dy, dx = q
            if not dy:
                add(name, fine, source, target, q, columns_of(fine, dx, depth), own, paths)
            elif not dx:
                add(name, fine, source, target, q, (fine.halo, fine.halo, fine.columns), [fine_rows(dy, depth)])
            else:
                add(name, fine, source, target, q, columns_of(fine, dx, corner), [fine_rows(dy, corner)])

    fine_set("u", u, u, 4, 3)
    fine_set("w", w, w, 3, 2, (1,))
    fine_set("f", f, f, 3, 2, (2,))
    fine_set("y", v, y, 3, 2, (1, 0, 2))
    for q in DIRS:
        dy, dx = q
        if not dy:
            add("near", coarse, cf, cf, q, columns_of(coarse, dx, 2), middle)
            for path, (count, skip) in enumerate(((5, 0), (4, 5), (4, 9))):
                add("cw", coarse, cw, cw, q, columns_of(coarse, dx, count, skip), middle, (path,))
            for path, skip in enumerate((2, 6, 10)):
                add("far", coarse, cf, cf, q, columns_of(coarse, dx, 4, skip), middle, (path,))
        elif not dx:
            place = coarse_rows(dy, LEVELS - 1)
            add("cw", coarse, cw, cw, q, (coarse.halo, coarse.halo, coarse.columns), place)
            place = coarse_rows(dy, LEVELS)
            at = coarse.halo + side(coarse.columns - 2, 0)
            add("near", coarse, cf, cf, q, (at, at, 2), place)
            at = coarse.halo + side(0, 2)
            add("far", coarse, cf, cf, q, (at, at, coarse.columns - 2), place)
        else:
            for count, skip, depth in ((2, 0, 12), (3, 2, 10), (4, 5, 7), (3, 9, 3)):
                add("cw", coarse, cw, cw, q, columns_of(coarse, dx, count, skip), coarse_rows(dy, depth))
            for count, skip, depth in ((2, 0, 13), (3, 2, 11), (4, 5, 8), (4, 9, 4)):
                name = "far" if skip else "near"
                add(name, coarse, cf, cf, q, columns_of(coarse, dx, count, skip), coarse_rows(dy, depth))

    first = {}
    for key in sorted(copies, key=lambda k: (k[0], DIRS.index(k[1]))):
        first[key] = counter[0]
        counter[0] += len(copies[key])

    def copies_of(name, q, arriving):
        back = (-q[0], -q[1])
        for i, (here, there, path, relay) in enumerate(copies[name, back if arriving else q]):
            yield path, pltpu.make_async_remote_copy(
                src_ref=here,
                dst_ref=there,
                send_sem=send_sem.at[first[name, q] + i],
                recv_sem=recv_sem.at[first[name, q if arriving else back] + i],
                device_id=name_of(q),
                device_id_type=MESH,
            )

    def legs_of(name, q):
        back = (-q[0], -q[1])
        for i, (here, there, path, relay) in enumerate(copies[name, q]):
            if path:
                yield path, pltpu.make_async_remote_copy(
                    src_ref=here,
                    dst_ref=relay,
                    send_sem=send_sem.at[first[name, q] + i],
                    recv_sem=land_sem.at[first[name, q] + i],
                    device_id={"lane": relays[q][path]},
                    device_id_type=MESH,
                ), pltpu.make_async_remote_copy(
                    src_ref=relay,
                    dst_ref=there,
                    send_sem=pass_sem.at[first[name, q] + i],
                    recv_sem=recv_sem.at[first[name, back] + i],
                    device_id={"lane": ends[q][1]},
                    device_id_type=MESH,
                )

    def start(name, q, when=None):
        ready = exists(q) if when is None else exists(q) & when
        direct = ready
        if any(path for *_, path, relay in copies[name, q]):
            direct = ready & (lane != ends[q][0])

            @pl.when(ready & (lane == ends[q][0]))
            def _():
                for path, copy in copies_of(name, q, False):
                    if not path:
                        copy.start()
                for path, there, on in legs_of(name, q):
                    there.start()

        @pl.when(direct)
        def _():
            for path, copy in copies_of(name, q, False):
                copy.start()

    def pass_on(names, finish=False):
        for q in ends:
            for way, relay_lane in relays[q].items():
                @pl.when(lane == relay_lane)
                def _():
                    for name in names:
                        for path, there, on in legs_of(name, q):
                            if path == way and finish:
                                on.wait_send()
                            elif path == way:
                                there.wait_recv()
                                on.start()

    def sent(names):
        for name in names:
            for q in DIRS:
                @pl.when(exists(q))
                def _():
                    for path, copy in copies_of(name, q, False):
                        copy.wait_send()

    def arrived(names, q, when=None):
        @pl.when(exists(q) if when is None else exists(q) & when)
        def _():
            for name in names:
                for path, copy in copies_of(name, q, True):
                    copy.wait_recv()

    rows_only, sides, corners = DIRS[:2], DIRS[2:4], DIRS[4:]

    def early_arrived(names):
        for q in rows_only:
            arrived(names, q)
        for q in sides + corners:
            arrived(names, q, jnp.logical_not(late(q)))

    def late_arrived(names):
        for q in sides + corners:
            arrived(names, q, late(q))

    def get(g, ref, column, p):
        return ref[pl.ds(g.at(column, p), SUB), :]

    def stencil(g, old, column, p, count):
        here = [get(g, old, column + j, p) for j in range(-1, count + 1)]
        found = []
        for j in range(count):
            up = get(g, old, column + j, p - 1) if p else pltpu.roll(get(g, old, column + j, g.pieces - 1), 1, 0)
            if p < g.pieces - 1:
                down = get(g, old, column + j, p + 1)
            else:
                down = pltpu.roll(get(g, old, column + j, 0), SUB - 1, 0)
            found.append((here[j + 1], (up + down) + (here[j] + here[j + 2])))
        return found

    def sweep(g, old, new, weight, load, at, blocks):
        @pl.loop(0, blocks)
        def _(b):
            column = at + BLOCK * b
            for p in range(g.pieces):
                for j, (here, total) in enumerate(stencil(g, old, column, p, BLOCK)):
                    c = column + j
                    value = 0.2 * here + get(g, load, c, p) + get(g, weight, c, p) * total
                    if new is out:
                        new[pl.ds(p * PITCH + c + MARGIN, SUB, stride=g.pieces * PITCH), :] = value
                    else:
                        new[pl.ds(g.at(c, p), SUB), :] = value

    def natural(ref, column, i):
        return ref[pl.ds((column + coarse.halo) * coarse.width + 2 + i, SUB, stride=coarse.pieces), :]

    def put_natural(ref, column, i, value):
        ref[pl.ds((column + coarse.halo) * coarse.width + 2 + i, SUB, stride=coarse.pieces), :] = value

    def paired(slot, i):
        at = slot * 96 + 16 * i + TOP
        return sums[pl.ds(at, SUB, stride=2), :] + sums[pl.ds(at + 1, SUB, stride=2), :]

    def restrict(at, blocks):
        @pl.loop(0, blocks)
        def _(b):
            column = at + RATIO * b
            for p in range(fine.pieces):
                found = stencil(fine, v, RATIO * column, p, BLOCK)
                defects = []
                for j, (here, total) in enumerate(found):
                    c = RATIO * column + j
                    change = get(fine, f, c, p) + get(fine, w, c, p) * total - 0.8 * here
                    defects.append(change * get(fine, iw, c, p))
                for slot in range(2):
                    sums[pl.ds(slot * 96 + p, SUB, stride=fine.pieces), :] = defects[2 * slot] + defects[2 * slot + 1]
            for slot in range(2):
                for i in range(4):
                    put_natural(
                        cf, column + slot, i, (paired(slot, i) * (1.0 / RATIO)) * natural(cw, column + slot, i)
                    )

    def correct(values, at, blocks):
        @pl.loop(0, blocks)
        def _(b):
            column = at + RATIO * b
            for slot in range(2):
                for i in range(-1, 5):
                    more = natural(values, column + slot, i)
                    place = slot * 96 + 16 * (i + 1)
                    sums[pl.ds(place, SUB, stride=2), :] = more
                    sums[pl.ds(place + 1, SUB, stride=2), :] = more
            for slot in range(2):
                for p in range(fine.pieces):
                    more = sums[pl.ds(slot * 96 + CTOP - TOP + p, SUB, stride=fine.pieces), :]
                    for j in range(RATIO):
                        c = fine.at(RATIO * (column + slot) + j, p)
                        v[pl.ds(c, SUB), :] = v[pl.ds(c, SUB), :] + more

    loaded(0)
    loaded(1)

    @pl.loop(0, fine.columns)
    def _(c):
        for p in range(fine.pieces):
            s, n = (1, 7) if p < 4 else (0, 8) if p == 4 else (0, 7)
            at = (c + fine.halo) * fine.width + p * SUB + s
            g4 = 4.0 + ra[pl.ds(at, n), :]
            weight = 0.8 / g4
            w[pl.ds(at, n), :] = weight
            f[pl.ds(at, n), :] = weight * rs[pl.ds(at, n), :]
            iw[pl.ds(at, n), :] = 1.25 * g4

    @pl.loop(0, coarse.columns // 2)
    def _(b):
        for slot in range(2):
            c = RATIO * (2 * b + slot)
            for p in range(fine.pieces):
                total = (4.0 + get(fine, ra, c, p)) + (4.0 + get(fine, ra, c + 1, p))
                sums[pl.ds(slot * 96 + p, SUB, stride=fine.pieces), :] = total
        for slot in range(2):
            for i in range(4):
                mean = paired(slot, i) * (1.0 / RATIO) - (4.0 * RATIO - 4.0)
                put_natural(cw, 2 * b + slot, i, 0.8 / mean)

    loaded(2)
    on_band = (band > 0).astype(jnp.int32) + (band < bands - 1).astype(jnp.int32)
    on_lane = (lane > 0).astype(jnp.int32) + (lane < lanes - 1).astype(jnp.int32)
    on_leg = sum((lane == source).astype(jnp.int32) for source, target in legs)
    pl.semaphore_wait(barrier, (on_band + 1) * (on_lane + 1) - 1 + on_leg)

    for name in ("u", "w", "f"):
        for q in sides:
            start(name, q)
    for name in ("u", "w", "f"):
        for q in corners:
            start(name, q)
    for name in ("u", "w", "f"):
        for q in rows_only:
            start(name, q)
    for q in sides + corners + rows_only:
        start("cw", q)
    pass_on(("w", "f"))

    before = ((u, v), (v, x), (x, v))
    early_arrived(("u", "w", "f"))
    for k, (old, new) in enumerate(before, 1):
        width = 4 * -(-(68 - 2 * k) // 4)
        sweep(fine, old, new, w, f, side(64 - k - width, k), width // 4)
    restrict(side(0, 2), 15)
    for q in sides + corners:
        start("far", q)
    for q in sides + corners:
        start("near", q, jnp.logical_not(late(q)))
    for q in rows_only:
        start("far", q)
    late_arrived(("u", "w", "f"))
    for k, (old, new) in enumerate(before, 1):
        sweep(fine, old, new, w, f, side(64 - k, k - 4), 1)
    restrict(side(30, 0), 1)
    for q in sides + corners:
        start("near", q, late(q))
    for q in rows_only:
        start("near", q)
    for q in sides + corners + rows_only:
        start("y", q)

    pass_on(("cw", "far", "y"))

    inner = []
    old = cf
    for k in range(2, INNER + 1):
        new = ca if k % 2 == 0 else cb
        inner.append((k, old, new))
        old = new
    sent(("u", "w", "f", "cw"))
    early_arrived(("cw", "far", "near"))
    for k, old, new in inner:
        width = 4 * -(-(48 - 2 * k) // 4)
        sweep(coarse, old, new, cw, cf, side(33 - k - width, k - 1), width // 4)

    last = inner[-1][2]
    after = ((v, u), (u, v), (v, out))

    def take(column):
        @pl.loop(0, 3)
        def _(j):
            for p in range(fine.pieces):
                at = fine.at(column + j, p)
                v[pl.ds(at, SUB), :] = y[pl.ds(at, SUB), :]

    def deliver(at):
        @pl.loop(0, rows)
        def _(row):
            for i in range(4):
                c = pl.multiple_of(at + SUB * i, SUB)
                place = pl.multiple_of((row + TOP) * PITCH + MARGIN + c, SUB)
                out_ref[row, pl.ds(c, SUB), :] = out[pl.ds(place, SUB), :]

    sent(("y", "far", "near"))
    pass_on(("w", "f", "cw", "far", "y"), finish=True)
    early_arrived(("y",))

    @pl.loop(0, fine.columns // SUB)
    def _(j):
        for p, s in ((1, 0), (2, 0), (3, 0), (5, 7), (6, 7), (7, 7)):
            at = (j * SUB + fine.halo) * fine.width + p * SUB + s
            v[pl.ds(at, SUB, stride=fine.width), :] = y[pl.ds(at, SUB, stride=fine.width), :]

    take(side(-3, 64))
    correct(last, side(-2, 12), 11)
    for m, (old, new) in enumerate(after, 1):
        width = 4 * -(-(43 - 2 * m) // 4)
        sweep(fine, old, new, w, f, side(40 - m - width, 24 + m), width // 4)
    deliver(side(0, 32))

    late_arrived(("cw", "far", "near"))
    for k, old, new in inner:
        sweep(coarse, old, new, cw, cf, side(33 - k, k - 17), 4)
    late_arrived(("y",))
    take(side(64, -3))
    correct(last, side(20, -2), 7)
    for m, (old, new) in enumerate(after, 1):
        sweep(fine, old, new, w, f, side(40 - m, m - 4), 7)
    deliver(side(32, 0))


def per_device(source_terms, initial_values, absorption):
    rows, columns, cases = source_terms.shape
    fine = Grid(columns, (rows + 2 * TOP) // SUB, 8)
    coarse = Grid(columns // RATIO, (rows // RATIO + 2 * CTOP) // SUB, 18)

    def held(*shape):
        return pltpu.VMEM(shape + (cases,), jnp.float32)

    shapes = [held(fine.stored * fine.width) for _ in range(9)]
    shapes += [held(coarse.stored * coarse.width) for _ in range(4)]
    shapes += [held((rows + 2 * TOP) * PITCH), held(2 * 96)]
    shapes += [held(12 * fine.width), held(8 * coarse.width)]
    count = 144
    shapes += [
        pltpu.SemaphoreType.DMA((3,)),
        pltpu.SemaphoreType.DMA((count,)),
        pltpu.SemaphoreType.DMA((count,)),
        pltpu.SemaphoreType.DMA((count,)),
        pltpu.SemaphoreType.DMA((count,)),
    ]
    return pl.pallas_call(
        functools.partial(kernel, fine, coarse),
        out_shape=jax.ShapeDtypeStruct(source_terms.shape, jnp.float32),
        in_specs=[pl.BlockSpec(memory_space=pltpu.HBM)] * 3,
        out_specs=pl.BlockSpec(memory_space=pltpu.VMEM),
        scratch_shapes=shapes,
        compiler_params=pltpu.CompilerParams(
            collective_id=0, has_side_effects=True, vmem_limit_bytes=52 * 1024 * 1024
        ),
    )(*[pltpu.with_memory_space_constraint(x, pltpu.HBM) for x in (source_terms, initial_values, absorption)])


def solution(mesh):
    placed = P(("shift", "band"), "lane", None)
    return jax.shard_map(
        per_device,
        mesh=mesh,
        in_specs=(placed, placed, placed),
        out_specs=placed,
        check_vma=False,
    )
```

```python
import functools

import jax
import jax.numpy as jnp
from jax import lax
from jax.experimental import pallas as pl
from jax.experimental.pallas import tpu as pltpu
from jax.sharding import PartitionSpec as P

RATIO = 2
INNER = 13
SUB = 8
BLOCK = 4
MESH = pl.DeviceIdType.MESH
DIRS = [(-1, 0), (1, 0), (0, -1), (0, 1), (-1, -1), (-1, 1), (1, -1), (1, 1)]
TOP = 4
CTOP = 16
LEVELS = 14
PITCH = 88
MARGIN = 8


class Grid:
    def __init__(self, columns, pieces, halo):
        self.columns, self.pieces, self.halo = columns, pieces, halo
        self.width = pieces * SUB
        self.stored = columns + 2 * halo

    def at(self, column, piece=0):
        return pl.multiple_of((column + self.halo) * self.width + piece * SUB, SUB)

    def boxes(self, ref):
        return ref.reshape(self.stored, self.pieces, SUB, 128)


def deliver(held, out_hbm, sem):
    rows, columns, _ = out_hbm.shape
    whole = held.reshape(rows + 2 * TOP, PITCH, 128).at[pl.ds(TOP, rows), pl.ds(MARGIN, columns), :]
    copy = pltpu.make_async_copy(whole, out_hbm, sem)
    copy.start()
    copy.wait()


def kernel(fine, coarse, src_hbm, init_hbm, abs_hbm, out, *scratch):
    u, v, x, w, f, y, iw, ra, rs, cw, cf, ca, cb, sums, fine_relay, coarse_relay, in_sem, send_sem, recv_sem, pass_sem, land_sem = scratch
    band, lane = lax.axis_index("band"), lax.axis_index("lane")
    bands, lanes = lax.axis_size("band"), lax.axis_size("lane")
    rows = fine.columns
    right = lane < lanes // 2

    def exists(q):
        dy, dx = q
        there = None
        if dy:
            there = (band > 0) if dy < 0 else (band < bands - 1)
        if dx:
            beside = (lane > 0) if dx < 0 else (lane < lanes - 1)
            there = beside if not dy else there & beside
        return there

    def name_of(q):
        return {"band": band + q[0], "lane": lane + q[1]}

    def late(q):
        return right if q[1] > 0 else jnp.logical_not(right)

    def side(if_right, if_left):
        return jnp.where(right, if_right, if_left)

    low, high = lanes // 2 - 1, lanes // 2
    ends = {(0, 1): (low, high), (0, -1): (high, low)}
    relays = {
        (0, 1): {1: lanes // 4 - 1, 2: 0, 3: lanes // 4},
        (0, -1): {1: lanes - lanes // 4, 2: lanes - 1, 3: lanes - lanes // 4 - 1},
    }
    legs = []
    for q, (source, target) in ends.items():
        for relay in relays[q].values():
            legs += [(source, relay), (relay, source), (relay, target), (target, relay)]

    barrier = pltpu.get_barrier_semaphore()
    for q in DIRS:
        @pl.when(exists(q))
        def _():
            pl.semaphore_signal(barrier, inc=1, device_id=name_of(q), device_id_type=MESH)
    for source, target in legs:
        @pl.when(lane == source)
        def _():
            pl.semaphore_signal(barrier, inc=1, device_id={"lane": target}, device_id_type=MESH)

    inputs = ((abs_hbm, ra), (src_hbm, rs), (init_hbm, u))
    for i, (ref, held) in enumerate(inputs):
        @pl.loop(0, rows)
        def _(row):
            at = row + TOP
            place = (at % fine.pieces) * SUB + at // fine.pieces
            to = held.reshape(fine.stored, fine.width, 128).at[
                pl.ds(fine.halo, fine.columns), pl.ds(place, 1), :
            ]
            pltpu.make_async_copy(ref.at[row].reshape(fine.columns, 1, 128), to, in_sem.at[i]).start()

    def loaded(i):
        ref, held = inputs[i]
        whole = held.reshape(fine.stored, fine.width, 128).at[pl.ds(fine.halo, fine.columns), pl.ds(0, rows), :]
        pltpu.make_async_copy(ref, whole, in_sem.at[i]).wait()

    zero = jnp.zeros((SUB, 128), jnp.float32)
    for dx in (-1, 1):
        @pl.when(jnp.logical_not(exists((0, dx))))
        def _():
            for g, refs, depth in ((fine, (u, w, f, y), 4), (coarse, (cw, cf), LEVELS)):
                @pl.loop(0, depth)
                def _(j):
                    column = j - depth if dx < 0 else g.columns + j
                    for ref in refs:
                        for p in range(g.pieces):
                            ref[pl.ds(g.at(column, p), SUB), :] = zero

    for dy in (-1, 1):
        @pl.when(jnp.logical_not(exists((dy, 0))))
        def _():
            @pl.loop(0, fine.stored // SUB)
            def _(j):
                for ref in (u, w, f, y):
                    for p in range(TOP):
                        place = p * SUB if dy < 0 else (fine.pieces - 1 - p) * SUB + SUB - 1
                        ref[pl.ds(j * SUB * fine.width + place, SUB, stride=fine.width), :] = zero

            @pl.loop(0, coarse.stored)
            def _(j):
                for ref in (cw, cf):
                    for p in range(coarse.pieces):
                        at = coarse.width * j + p * SUB + (0 if dy < 0 else SUB - 2)
                        ref[pl.ds(at, 2), :] = zero[:2]

    def columns_of(g, dx, depth, skip=0):
        if dx > 0:
            return g.halo + g.columns - depth - skip, g.halo - depth - skip, depth
        return g.halo + skip, g.halo + g.columns + skip, depth

    def fine_rows(dy, depth, skip=0):
        if dy > 0:
            return [((5 - depth - skip, 7), (4 - depth - skip, 0), (depth, 1))]
        return [((4 + skip, 0), (5 + skip, 7), (depth, 1))]

    def coarse_rows(dy, depth):
        e = depth - SUB
        if e <= 0:
            if dy > 0:
                return [((SUB - depth, 5), (SUB - depth, 1), (depth, 1))]
            return [((0, 2), (0, 6), (depth, 1))]
        if dy > 0:
            return [((SUB - e, 4), (SUB - e, 0), (e, 2)), ((0, 5), (0, 1), (SUB - e, 1))]
        return [((0, 2), (0, 6), (e, 2)), ((e, 2), (e, 6), (SUB - e, 1))]

    own = [((0, 1), (0, 1), (4, 7)), ((4, 0), (4, 0), (1, 8)), ((5, 0), (5, 0), (4, 7))]
    middle = [((0, 2), (0, 2), (SUB, 4))]

    copies, used, volume = {}, {}, {}
    offsets = {"w": 0, "f": 3, "y": 9, "cw": 0, "far": 3}

    def add(name, g, source, target, q, columns, places, paths=(0,)):
        from_column, to_column, count = columns
        for i, ((p, s), (pt, st), (np_, ns)) in enumerate(places):
            here = g.boxes(source).at[pl.ds(from_column, count), pl.ds(p, np_), pl.ds(s, ns), :]
            there = g.boxes(target).at[pl.ds(to_column, count), pl.ds(pt, np_), pl.ds(st, ns), :]
            path = paths[i % len(paths)]
            relay = None
            if path:
                held = fine_relay if g is fine else coarse_relay
                base = used.setdefault((name, q, path), 0)
                used[name, q, path] = base + count
                base += offsets[name]
                relay = held.reshape(held.shape[0] // g.width, g.pieces, SUB, 128).at[
                    pl.ds(base, count), pl.ds(p, np_), pl.ds(s, ns), :
                ]
            copies.setdefault((name, q), []).append((here, there, path, relay))
            volume[name, q, path] = volume.get((name, q, path), 0) + count * np_ * ns

    for q in DIRS:
        dy, dx = q
        for name, source, target, depth, corner in (("u", u, u, 4, 3), ("w", w, w, 3, 2), ("f", f, f, 3, 2)):
            if not dy and name == "u":
                add(name, fine, source, target, q, columns_of(fine, dx, depth), own)
            elif not dy:
                path = 1 if name == "w" else 2
                add(name, fine, source, target, q, columns_of(fine, dx, 2), own, (path,))
                add(name, fine, source, target, q, columns_of(fine, dx, 1, 2), own, (3,))
            elif not dx:
                add(name, fine, source, target, q, (fine.halo, fine.halo, fine.columns), fine_rows(dy, depth))
            else:
                add(name, fine, source, target, q, columns_of(fine, dx, corner), fine_rows(dy, corner))
        if not dy:
            add("y", fine, v, y, q, columns_of(fine, dx, 2, 1), own, (1, 0, 3))
        elif not dx:
            add("y", fine, v, y, q, (fine.halo, fine.halo, fine.columns), fine_rows(dy, 2, 1))
        else:
            add("y", fine, v, y, q, columns_of(fine, dx, 2), fine_rows(dy, 2))

    for q in DIRS:
        dy, dx = q
        if not dy:
            add("near", coarse, cf, cf, q, columns_of(coarse, dx, 2), middle)
            for path, (count, skip) in enumerate(((4, 0), (3, 4), (3, 7), (3, 10))):
                add("cw", coarse, cw, cw, q, columns_of(coarse, dx, count, skip), middle, (path,))
            for path, skip in enumerate((2, 5, 8, 11)):
                add("far", coarse, cf, cf, q, columns_of(coarse, dx, 3, skip), middle, (path,))
        elif not dx:
            place = coarse_rows(dy, LEVELS - 1)
            add("cw", coarse, cw, cw, q, (coarse.halo, coarse.halo, coarse.columns), place)
            place = coarse_rows(dy, LEVELS)
            at = coarse.halo + side(coarse.columns - 2, 0)
            add("near", coarse, cf, cf, q, (at, at, 2), place)
            at = coarse.halo + side(0, 2)
            add("far", coarse, cf, cf, q, (at, at, coarse.columns - 2), place)
        else:
            for count, skip, depth in ((2, 0, 12), (3, 2, 10), (4, 5, 7), (3, 9, 3)):
                add("cw", coarse, cw, cw, q, columns_of(coarse, dx, count, skip), coarse_rows(dy, depth))
            for count, skip, depth in ((2, 0, 13), (3, 2, 11), (4, 5, 8), (4, 9, 4)):
                name = "far" if skip else "near"
                add(name, coarse, cf, cf, q, columns_of(coarse, dx, count, skip), coarse_rows(dy, depth))

    groups = (("u", "w", "f"), ("cw", "far", "near"), ("y",))
    relayed = ("w", "f", "cw", "far", "y")

    def place_of(name, q):
        group = [name in names for names in groups].index(True)
        return group * len(DIRS) + DIRS.index(q)

    def wait(sem, count):
        rows_of = u.at[pl.ds(0, count), :]
        pltpu.make_async_copy(rows_of, rows_of, sem).wait()

    def total(names, q, path=None):
        return sum(n for (name, d, way), n in volume.items() if name in names and d == q and path in (None, way))

    def copies_of(name, q):
        back = (-q[0], -q[1])
        for here, there, path, relay in copies[name, q]:
            yield path, pltpu.make_async_remote_copy(
                src_ref=here,
                dst_ref=there,
                send_sem=send_sem.at[place_of(name, q)],
                recv_sem=recv_sem.at[place_of(name, back)],
                device_id=name_of(q),
                device_id_type=MESH,
            )

    def legs_of(name, q, way=None):
        back = (-q[0], -q[1])
        for here, there, path, relay in copies[name, q]:
            if path and way in (None, path):
                yield pltpu.make_async_remote_copy(
                    src_ref=here,
                    dst_ref=relay,
                    send_sem=send_sem.at[place_of(name, q)],
                    recv_sem=land_sem.at[relayed.index(name)],
                    device_id={"lane": relays[q][path]},
                    device_id_type=MESH,
                ), pltpu.make_async_remote_copy(
                    src_ref=relay,
                    dst_ref=there,
                    send_sem=pass_sem.at[0],
                    recv_sem=recv_sem.at[place_of(name, back)],
                    device_id={"lane": ends[q][1]},
                    device_id_type=MESH,
                )

    def start(name, q, when=None):
        ready = exists(q) if when is None else exists(q) & when
        direct = ready
        if any(path for *_, path, relay in copies[name, q]):
            direct = ready & (lane != ends[q][0])

            @pl.when(ready & (lane == ends[q][0]))
            def _():
                for there, on in legs_of(name, q):
                    there.start()
                for path, copy in copies_of(name, q):
                    if not path:
                        copy.start()

        @pl.when(direct)
        def _():
            for path, copy in copies_of(name, q):
                copy.start()

    def pass_on(names):
        for q in ends:
            for way, relay_lane in relays[q].items():
                @pl.when(lane == relay_lane)
                def _():
                    for name in names:
                        if total((name,), q, way):
                            wait(land_sem.at[relayed.index(name)], total((name,), q, way))
                            for there, on in legs_of(name, q, way):
                                on.start()

    def passed_on():
        for q in ends:
            for way, relay_lane in relays[q].items():
                @pl.when(lane == relay_lane)
                def _():
                    wait(pass_sem.at[0], total(relayed, q, way))

    def sent(names):
        for q in DIRS:
            @pl.when(exists(q))
            def _():
                wait(send_sem.at[place_of(names[0], q)], total(names, q))

    def arrived(names, q, when=None):
        @pl.when(exists(q) if when is None else exists(q) & when)
        def _():
            wait(recv_sem.at[place_of(names[0], q)], total(names, (-q[0], -q[1])))

    rows_only, sides, corners = DIRS[:2], DIRS[2:4], DIRS[4:]

    def early_arrived(names):
        for q in rows_only:
            arrived(names, q)
        for q in sides + corners:
            arrived(names, q, jnp.logical_not(late(q)))

    def late_arrived(names):
        for q in sides + corners:
            arrived(names, q, late(q))

    def get(g, ref, column, p):
        return ref[pl.ds(g.at(column, p), SUB), :]

    def stencil(g, old, column, p, count):
        here = [get(g, old, column + j, p) for j in range(-1, count + 1)]
        found = []
        for j in range(count):
            up = get(g, old, column + j, p - 1) if p else pltpu.roll(get(g, old, column + j, g.pieces - 1), 1, 0)
            if p < g.pieces - 1:
                down = get(g, old, column + j, p + 1)
            else:
                down = pltpu.roll(get(g, old, column + j, 0), SUB - 1, 0)
            found.append((here[j + 1], (up + down) + (here[j] + here[j + 2])))
        return found

    def sweep(g, old, new, weight, load, at, blocks):
        @pl.loop(0, blocks)
        def _(b):
            column = at + BLOCK * b
            for p in range(g.pieces):
                for j, (here, total) in enumerate(stencil(g, old, column, p, BLOCK)):
                    c = column + j
                    value = 0.2 * here + get(g, load, c, p) + get(g, weight, c, p) * total
                    if new is out:
                        new[pl.ds(p * PITCH + c + MARGIN, SUB, stride=g.pieces * PITCH), :] = value
                    else:
                        new[pl.ds(g.at(c, p), SUB), :] = value

    def natural(ref, column, i):
        return ref[pl.ds((column + coarse.halo) * coarse.width + 2 + i, SUB, stride=coarse.pieces), :]

    def put_natural(ref, column, i, value):
        ref[pl.ds((column + coarse.halo) * coarse.width + 2 + i, SUB, stride=coarse.pieces), :] = value

    def paired(slot, i):
        at = slot * 96 + 16 * i + TOP
        return sums[pl.ds(at, SUB, stride=2), :] + sums[pl.ds(at + 1, SUB, stride=2), :]

    def restrict(at, blocks):
        @pl.loop(0, blocks)
        def _(b):
            column = at + RATIO * b
            for p in range(fine.pieces):
                found = stencil(fine, v, RATIO * column, p, BLOCK)
                defects = []
                for j, (here, total) in enumerate(found):
                    c = RATIO * column + j
                    change = get(fine, f, c, p) + get(fine, w, c, p) * total - 0.8 * here
                    defects.append(change * get(fine, iw, c, p))
                for slot in range(2):
                    sums[pl.ds(slot * 96 + p, SUB, stride=fine.pieces), :] = defects[2 * slot] + defects[2 * slot + 1]
            for slot in range(2):
                for i in range(4):
                    put_natural(
                        cf, column + slot, i, (paired(slot, i) * (1.0 / RATIO)) * natural(cw, column + slot, i)
                    )

    def correct(values, at, blocks):
        @pl.loop(0, blocks)
        def _(b):
            column = at + RATIO * b
            for slot in range(2):
                for i in range(-1, 5):
                    more = natural(values, column + slot, i)
                    place = slot * 96 + 16 * (i + 1)
                    sums[pl.ds(place, SUB, stride=2), :] = more
                    sums[pl.ds(place + 1, SUB, stride=2), :] = more
            for slot in range(2):
                for p in range(fine.pieces):
                    more = sums[pl.ds(slot * 96 + CTOP - TOP + p, SUB, stride=fine.pieces), :]
                    for j in range(RATIO):
                        c = fine.at(RATIO * (column + slot) + j, p)
                        v[pl.ds(c, SUB), :] = v[pl.ds(c, SUB), :] + more

    loaded(0)
    loaded(1)

    @pl.loop(0, fine.columns)
    def _(c):
        for p in range(fine.pieces):
            s, n = (1, 7) if p < 4 else (0, 8) if p == 4 else (0, 7)
            at = (c + fine.halo) * fine.width + p * SUB + s
            g4 = 4.0 + ra[pl.ds(at, n), :]
            weight = 0.8 / g4
            w[pl.ds(at, n), :] = weight
            f[pl.ds(at, n), :] = weight * rs[pl.ds(at, n), :]
            iw[pl.ds(at, n), :] = 1.25 * g4

    @pl.loop(0, coarse.columns // 2)
    def _(b):
        for slot in range(2):
            c = RATIO * (2 * b + slot)
            for p in range(fine.pieces):
                total = (4.0 + get(fine, ra, c, p)) + (4.0 + get(fine, ra, c + 1, p))
                sums[pl.ds(slot * 96 + p, SUB, stride=fine.pieces), :] = total
        for slot in range(2):
            for i in range(4):
                mean = paired(slot, i) * (1.0 / RATIO) - (4.0 * RATIO - 4.0)
                put_natural(cw, 2 * b + slot, i, 0.8 / mean)

    loaded(2)
    on_band = (band > 0).astype(jnp.int32) + (band < bands - 1).astype(jnp.int32)
    on_lane = (lane > 0).astype(jnp.int32) + (lane < lanes - 1).astype(jnp.int32)
    on_leg = sum((lane == source).astype(jnp.int32) for source, target in legs)
    pl.semaphore_wait(barrier, (on_band + 1) * (on_lane + 1) - 1 + on_leg)

    for name in ("u", "w", "f"):
        for q in sides:
            start(name, q)
    for name in ("u", "w", "f"):
        for q in corners:
            start(name, q)
    for name in ("u", "w", "f"):
        for q in rows_only:
            start(name, q)
    for q in sides + corners + rows_only:
        start("cw", q)
    pass_on(("w", "f"))

    before = ((u, v), (v, x), (x, v))
    early_arrived(groups[0])
    for k, (old, new) in enumerate(before, 1):
        width = 4 * -(-(68 - 2 * k) // 4)
        sweep(fine, old, new, w, f, side(64 - k - width, k), width // 4)
    restrict(side(0, 2), 15)
    for q in sides + corners:
        start("far", q)
    for q in sides + corners:
        start("near", q, jnp.logical_not(late(q)))
    for q in rows_only:
        start("far", q)
    late_arrived(groups[0])
    for k, (old, new) in enumerate(before, 1):
        sweep(fine, old, new, w, f, side(64 - k, k - 4), 1)
    restrict(side(30, 0), 1)
    for q in sides + corners:
        start("near", q, late(q))
    for q in rows_only:
        start("near", q)
    for q in sides + corners + rows_only:
        start("y", q)

    pass_on(("cw", "far", "y"))

    inner = []
    old = cf
    for k in range(2, INNER + 1):
        new = ca if k % 2 == 0 else cb
        inner.append((k, old, new))
        old = new
    sent(groups[0])
    early_arrived(groups[1])
    for k, old, new in inner:
        width = 4 * -(-(48 - 2 * k) // 4)
        sweep(coarse, old, new, cw, cf, side(33 - k - width, k - 1), width // 4)

    last = inner[-1][2]
    after = ((v, u), (u, v), (v, out))

    def take(outer, inner):
        @pl.loop(0, 2)
        def _(j):
            for p in range(fine.pieces):
                at = fine.at(outer + j, p)
                v[pl.ds(at, SUB), :] = y[pl.ds(at, SUB), :]

        for p, s in ((2, 0), (3, 0), (5, 7), (6, 7)):
            at = (inner + fine.halo) * fine.width + p * SUB + s
            v[pl.ds(at, 1), :] = y[pl.ds(at, 1), :]

    sent(groups[1])
    sent(groups[2])
    passed_on()
    early_arrived(groups[2])

    @pl.loop(0, fine.columns // SUB)
    def _(j):
        for p, s in ((1, 0), (2, 0), (6, 7), (7, 7)):
            at = (j * SUB + fine.halo) * fine.width + p * SUB + s
            v[pl.ds(at, SUB, stride=fine.width), :] = y[pl.ds(at, SUB, stride=fine.width), :]

    take(side(-3, 65), side(-1, 64))
    correct(last, side(-2, 12), 11)
    for m, (old, new) in enumerate(after, 1):
        width = 4 * -(-(43 - 2 * m) // 4)
        sweep(fine, old, new, w, f, side(40 - m - width, 24 + m), width // 4)

    late_arrived(groups[1])
    for k, old, new in inner:
        sweep(coarse, old, new, cw, cf, side(33 - k, k - 17), 4)
    late_arrived(groups[2])
    take(side(65, -3), side(64, -1))
    correct(last, side(20, -2), 7)
    for m, (old, new) in enumerate(after, 1):
        sweep(fine, old, new, w, f, side(40 - m, m - 4), 7)


def per_device(source_terms, initial_values, absorption):
    rows, columns, cases = source_terms.shape
    fine = Grid(columns, (rows + 2 * TOP) // SUB, 8)
    coarse = Grid(columns // RATIO, (rows // RATIO + 2 * CTOP) // SUB, 18)

    def held(*shape):
        return pltpu.VMEM(shape + (cases,), jnp.float32)

    shapes = [held(fine.stored * fine.width) for _ in range(9)]
    shapes += [held(coarse.stored * coarse.width) for _ in range(4)]
    shapes += [held(2 * 96)]
    shapes += [held(11 * fine.width), held(6 * coarse.width)]
    shapes += [
        pltpu.SemaphoreType.DMA((3,)),
        pltpu.SemaphoreType.DMA((3 * len(DIRS),)),
        pltpu.SemaphoreType.DMA((3 * len(DIRS),)),
        pltpu.SemaphoreType.DMA((1,)),
        pltpu.SemaphoreType.DMA((5,)),
    ]
    pitched = pl.pallas_call(
        functools.partial(kernel, fine, coarse),
        out_shape=jax.ShapeDtypeStruct(((rows + 2 * TOP) * PITCH, cases), jnp.float32),
        in_specs=[pl.BlockSpec(memory_space=pltpu.HBM)] * 3,
        out_specs=pl.BlockSpec(memory_space=pltpu.VMEM),
        scratch_shapes=shapes,
        compiler_params=pltpu.CompilerParams(
            collective_id=0, has_side_effects=True, vmem_limit_bytes=52 * 1024 * 1024
        ),
    )(*[pltpu.with_memory_space_constraint(x, pltpu.HBM) for x in (source_terms, initial_values, absorption)])
    return pl.pallas_call(
        deliver,
        out_shape=jax.ShapeDtypeStruct(source_terms.shape, jnp.float32),
        in_specs=[pl.BlockSpec(memory_space=pltpu.VMEM)],
        out_specs=pl.BlockSpec(memory_space=pltpu.HBM),
        scratch_shapes=[pltpu.SemaphoreType.DMA],
    )(pitched)


def solution(mesh):
    placed = P(("shift", "band"), "lane", None)
    return jax.shard_map(
        per_device,
        mesh=mesh,
        in_specs=(placed, placed, placed),
        out_specs=placed,
        check_vma=False,
    )
```

```python
import functools

import jax
import jax.numpy as jnp
from jax import lax
from jax.experimental import pallas as pl
from jax.experimental.pallas import tpu as pltpu
from jax.sharding import PartitionSpec as P

RATIO = 2
INNER = 13
SUB = 8
BLOCK = 4
MESH = pl.DeviceIdType.MESH
DIRS = [(-1, 0), (1, 0), (0, -1), (0, 1), (-1, -1), (-1, 1), (1, -1), (1, 1)]
TOP = 4
CTOP = 16
LEVELS = 14
PITCH = 88
MARGIN = 8


class Grid:
    def __init__(self, columns, pieces, halo):
        self.columns, self.pieces, self.halo = columns, pieces, halo
        self.width = pieces * SUB
        self.stored = columns + 2 * halo

    def at(self, column, piece=0):
        return pl.multiple_of((column + self.halo) * self.width + piece * SUB, SUB)

    def boxes(self, ref):
        return ref.reshape(self.stored, self.pieces, SUB, 128)


def deliver(held, out_hbm, sem):
    rows, columns, _ = out_hbm.shape
    whole = held.reshape(rows + 2 * TOP, PITCH, 128).at[pl.ds(TOP, rows), pl.ds(MARGIN, columns), :]
    copy = pltpu.make_async_copy(whole, out_hbm, sem)
    copy.start()
    copy.wait()


def kernel(fine, coarse, src_hbm, init_hbm, abs_hbm, out, *scratch):
    u, v, x, w, f, y, iw, ra, rs, cw, cf, ca, cb, sums, fine_relay, coarse_relay, in_sem, send_sem, recv_sem, pass_sem, land_sem = scratch
    band, lane = lax.axis_index("band"), lax.axis_index("lane")
    bands, lanes = lax.axis_size("band"), lax.axis_size("lane")
    rows = fine.columns
    right = lane < lanes // 2

    def exists(q):
        dy, dx = q
        there = None
        if dy:
            there = (band > 0) if dy < 0 else (band < bands - 1)
        if dx:
            beside = (lane > 0) if dx < 0 else (lane < lanes - 1)
            there = beside if not dy else there & beside
        return there

    def name_of(q):
        return {"band": band + q[0], "lane": lane + q[1]}

    def late(q):
        return right if q[1] > 0 else jnp.logical_not(right)

    def side(if_right, if_left):
        return jnp.where(right, if_right, if_left)

    low, high = lanes // 2 - 1, lanes // 2
    ends = {(0, 1): (low, high), (0, -1): (high, low)}
    relays = {
        (0, 1): {1: lanes // 4 - 1, 2: 0, 3: lanes // 4},
        (0, -1): {1: lanes - lanes // 4, 2: lanes - 1, 3: lanes - lanes // 4 - 1},
    }
    legs = []
    for q, (source, target) in ends.items():
        for relay in relays[q].values():
            legs += [(source, relay), (relay, source), (relay, target), (target, relay)]

    barrier = pltpu.get_barrier_semaphore()
    for q in DIRS:
        @pl.when(exists(q))
        def _():
            pl.semaphore_signal(barrier, inc=1, device_id=name_of(q), device_id_type=MESH)
    for source, target in legs:
        @pl.when(lane == source)
        def _():
            pl.semaphore_signal(barrier, inc=1, device_id={"lane": target}, device_id_type=MESH)

    inputs = ((abs_hbm, ra), (src_hbm, rs), (init_hbm, u))
    for i, (ref, held) in enumerate(inputs):
        @pl.loop(0, rows)
        def _(row):
            at = row + TOP
            place = (at % fine.pieces) * SUB + at // fine.pieces
            to = held.reshape(fine.stored, fine.width, 128).at[
                pl.ds(fine.halo, fine.columns), pl.ds(place, 1), :
            ]
            pltpu.make_async_copy(ref.at[row].reshape(fine.columns, 1, 128), to, in_sem.at[i]).start()

    def loaded(i):
        ref, held = inputs[i]
        whole = held.reshape(fine.stored, fine.width, 128).at[pl.ds(fine.halo, fine.columns), pl.ds(0, rows), :]
        pltpu.make_async_copy(ref, whole, in_sem.at[i]).wait()

    zero = jnp.zeros((SUB, 128), jnp.float32)
    for dx in (-1, 1):
        @pl.when(jnp.logical_not(exists((0, dx))))
        def _():
            for g, refs, depth in ((fine, (u, w, f, y), 4), (coarse, (cw, cf), LEVELS)):
                @pl.loop(0, depth)
                def _(j):
                    column = j - depth if dx < 0 else g.columns + j
                    for ref in refs:
                        for p in range(g.pieces):
                            ref[pl.ds(g.at(column, p), SUB), :] = zero

    for dy in (-1, 1):
        @pl.when(jnp.logical_not(exists((dy, 0))))
        def _():
            @pl.loop(0, fine.stored // SUB)
            def _(j):
                for ref in (u, w, f, y):
                    for p in range(TOP):
                        place = p * SUB if dy < 0 else (fine.pieces - 1 - p) * SUB + SUB - 1
                        ref[pl.ds(j * SUB * fine.width + place, SUB, stride=fine.width), :] = zero

            @pl.loop(0, coarse.stored)
            def _(j):
                for ref in (cw, cf):
                    for p in range(coarse.pieces):
                        at = coarse.width * j + p * SUB + (0 if dy < 0 else SUB - 2)
                        ref[pl.ds(at, 2), :] = zero[:2]

    def columns_of(g, dx, depth, skip=0):
        if dx > 0:
            return g.halo + g.columns - depth - skip, g.halo - depth - skip, depth
        return g.halo + skip, g.halo + g.columns + skip, depth

    def outside(g, dx, depth, skip):
        return g.halo + g.columns + skip if dx > 0 else g.halo - depth - skip

    def fine_rows(dy, depth, skip=0):
        if dy > 0:
            return [((5 - depth - skip, 7), (4 - depth - skip, 0), (depth, 1))]
        return [((4 + skip, 0), (5 + skip, 7), (depth, 1))]

    def coarse_rows(dy, depth):
        e = depth - SUB
        if e <= 0:
            if dy > 0:
                return [((SUB - depth, 5), (SUB - depth, 1), (depth, 1))]
            return [((0, 2), (0, 6), (depth, 1))]
        if dy > 0:
            return [((SUB - e, 4), (SUB - e, 0), (e, 2)), ((0, 5), (0, 1), (SUB - e, 1))]
        return [((0, 2), (0, 6), (e, 2)), ((e, 2), (e, 6), (SUB - e, 1))]

    own = [((0, 1), (0, 1), (4, 7)), ((4, 0), (4, 0), (1, 8)), ((5, 0), (5, 0), (4, 7))]
    middle = [((0, 2), (0, 2), (SUB, 4))]

    copies, used, volume = {}, {}, {}
    offsets = {"w": 0, "f": 9, "y": 18, "cw": 0, "far": 8}

    def add(name, g, source, target, q, columns, places, paths=(0,)):
        from_column, to_column, count = columns
        for i, ((p, s), (pt, st), (np_, ns)) in enumerate(places):
            here = g.boxes(source).at[pl.ds(from_column, count), pl.ds(p, np_), pl.ds(s, ns), :]
            there = g.boxes(target).at[pl.ds(to_column, count), pl.ds(pt, np_), pl.ds(st, ns), :]
            path = paths[i % len(paths)]
            relay = None
            if path:
                held = fine_relay if g is fine else coarse_relay
                base = used.setdefault((name, q, path), 0)
                used[name, q, path] = base + count
                base += offsets[name]
                relay = held.reshape(held.shape[0] // g.width, g.pieces, SUB, 128).at[
                    pl.ds(base, count), pl.ds(p, np_), pl.ds(s, ns), :
                ]
            copies.setdefault((name, q), []).append((here, there, path, relay))
            volume[name, q, path] = volume.get((name, q, path), 0) + count * np_ * ns

    for q in DIRS:
        dy, dx = q
        for name, source, target, depth, corner in (("u", u, u, 4, 3), ("w", w, w, 3, 2), ("f", f, f, 3, 2)):
            if not dy and name == "u":
                add(name, fine, source, target, q, columns_of(fine, dx, depth), own)
            elif not dy:
                add(name, fine, source, target, q, columns_of(fine, dx, 3), own, (2 if name == "w" else 2,))
            elif not dx:
                add(name, fine, source, target, q, (fine.halo, fine.halo, fine.columns), fine_rows(dy, depth))
            else:
                add(name, fine, source, target, q, columns_of(fine, dx, corner), fine_rows(dy, corner))
        if not dy:
            add("y", fine, v, y, q, columns_of(fine, dx, 2, 1), own, (2, 0, 2))
        elif not dx:
            add("y", fine, v, y, q, (fine.halo, fine.halo, fine.columns), fine_rows(dy, 2, 1))
        else:
            add("y", fine, v, y, q, columns_of(fine, dx, 2), fine_rows(dy, 2))

    for q in DIRS:
        dy, dx = q
        if not dy:
            add("near", coarse, cf, cf, q, columns_of(coarse, dx, 2), middle)
            for path, count, skip in ((0, 4, 0), (1, 3, 4), (2, 3, 7), (3, 3, 10)):
                add("cw", coarse, cw, cw, q, columns_of(coarse, dx, count, skip), middle, (path,))
            for path, count, skip in ((0, 3, 2), (1, 3, 5), (2, 3, 8), (3, 3, 11)):
                add("far", coarse, cf, cf, q, columns_of(coarse, dx, count, skip), middle, (path,))
        elif not dx:
            place = coarse_rows(dy, LEVELS - 1)
            add("cw", coarse, cw, cw, q, (coarse.halo, coarse.halo, coarse.columns), place)
            place = coarse_rows(dy, LEVELS)
            at = coarse.halo + side(coarse.columns - 2, 0)
            add("near", coarse, cf, cf, q, (at, at, 2), place)
            at = coarse.halo + side(0, 2)
            add("far", coarse, cf, cf, q, (at, at, coarse.columns - 2), place)
        else:
            add("near", coarse, cf, cf, q, columns_of(coarse, dx, 2), coarse_rows(dy, LEVELS - 1))
            for count, skip, depth in ((2, 0, 12), (3, 2, 10), (4, 5, 7), (3, 9, 3)):
                at = outside(coarse, dx, count, skip)
                add("turn", coarse, cw, cw, q, (at, at, count), coarse_rows(dy, depth))
            for count, skip, depth in ((3, 2, 11), (4, 5, 8), (4, 9, 4)):
                at = outside(coarse, dx, count, skip)
                add("turn", coarse, cf, cf, q, (at, at, count), coarse_rows(dy, depth))

    groups = (("u", "w", "f"), ("cw", "far"), ("y",), ("near",), ("turn",))
    relayed = ("w", "f", "cw", "far", "y")

    def place_of(name, q):
        group = [name in names for names in groups].index(True)
        return group * len(DIRS) + DIRS.index(q)

    def from_side(name, q):
        return (-q[0], q[1]) if name == "turn" else (-q[0], -q[1])

    def wait(sem, count):
        if not count:
            return
        rows_of = u.at[pl.ds(0, count), :]
        pltpu.make_async_copy(rows_of, rows_of, sem).wait()

    def total(names, q, path=None):
        return sum(n for (name, d, way), n in volume.items() if name in names and d == q and path in (None, way))

    def copies_of(name, q):
        for here, there, path, relay in copies[name, q]:
            yield path, pltpu.make_async_remote_copy(
                src_ref=here,
                dst_ref=there,
                send_sem=send_sem.at[place_of(name, q)],
                recv_sem=recv_sem.at[place_of(name, from_side(name, q))],
                device_id=name_of((q[0], 0) if name == "turn" else q),
                device_id_type=MESH,
            )

    def legs_of(name, q, way=None):
        back = (-q[0], -q[1])
        for here, there, path, relay in copies[name, q]:
            if path and way in (None, path):
                yield pltpu.make_async_remote_copy(
                    src_ref=here,
                    dst_ref=relay,
                    send_sem=send_sem.at[place_of(name, q)],
                    recv_sem=land_sem.at[relayed.index(name)],
                    device_id={"lane": relays[q][path]},
                    device_id_type=MESH,
                ), pltpu.make_async_remote_copy(
                    src_ref=relay,
                    dst_ref=there,
                    send_sem=pass_sem.at[0],
                    recv_sem=recv_sem.at[place_of(name, back)],
                    device_id={"lane": ends[q][1]},
                    device_id_type=MESH,
                )

    def start(name, q, when=None):
        ready = exists(q) if when is None else exists(q) & when
        direct = ready
        if any(path for *_, path, relay in copies[name, q]):
            direct = ready & (lane != ends[q][0])

            @pl.when(ready & (lane == ends[q][0]))
            def _():
                for there, on in legs_of(name, q):
                    there.start()
                for path, copy in copies_of(name, q):
                    if not path:
                        copy.start()

        @pl.when(direct)
        def _():
            for path, copy in copies_of(name, q):
                copy.start()

    def pass_on(names):
        for q in ends:
            for way, relay_lane in relays[q].items():
                @pl.when(lane == relay_lane)
                def _():
                    for name in names:
                        if total((name,), q, way):
                            wait(land_sem.at[relayed.index(name)], total((name,), q, way))
                            for there, on in legs_of(name, q, way):
                                on.start()

    def passed_on():
        for q in ends:
            for way, relay_lane in relays[q].items():
                @pl.when(lane == relay_lane)
                def _():
                    wait(pass_sem.at[0], total(relayed, q, way))

    def sent(names):
        for q in DIRS:
            @pl.when(exists(q))
            def _():
                wait(send_sem.at[place_of(names[0], q)], total(names, q))

    def arrived(names, q, when=None):
        @pl.when(exists(q) if when is None else exists(q) & when)
        def _():
            wait(recv_sem.at[place_of(names[0], q)], total(names, from_side(names[0], q)))

    rows_only, sides, corners = DIRS[:2], DIRS[2:4], DIRS[4:]

    def early_arrived(names):
        for q in rows_only:
            arrived(names, q)
        for q in sides + corners:
            arrived(names, q, jnp.logical_not(late(q)))

    def late_arrived(names):
        for q in sides + corners:
            arrived(names, q, late(q))

    def get(g, ref, column, p):
        return ref[pl.ds(g.at(column, p), SUB), :]

    def stencil(g, old, column, p, count):
        here = [get(g, old, column + j, p) for j in range(-1, count + 1)]
        found = []
        for j in range(count):
            up = get(g, old, column + j, p - 1) if p else pltpu.roll(get(g, old, column + j, g.pieces - 1), 1, 0)
            if p < g.pieces - 1:
                down = get(g, old, column + j, p + 1)
            else:
                down = pltpu.roll(get(g, old, column + j, 0), SUB - 1, 0)
            found.append((here[j + 1], (up + down) + (here[j] + here[j + 2])))
        return found

    def sweep(g, old, new, weight, load, at, blocks):
        @pl.loop(0, blocks)
        def _(b):
            column = at + BLOCK * b
            for p in range(g.pieces):
                for j, (here, total) in enumerate(stencil(g, old, column, p, BLOCK)):
                    c = column + j
                    value = 0.2 * here + get(g, load, c, p) + get(g, weight, c, p) * total
                    if new is out:
                        new[pl.ds(p * PITCH + c + MARGIN, SUB, stride=g.pieces * PITCH), :] = value
                    else:
                        new[pl.ds(g.at(c, p), SUB), :] = value

    def natural(ref, column, i):
        return ref[pl.ds((column + coarse.halo) * coarse.width + 2 + i, SUB, stride=coarse.pieces), :]

    def put_natural(ref, column, i, value):
        ref[pl.ds((column + coarse.halo) * coarse.width + 2 + i, SUB, stride=coarse.pieces), :] = value

    def paired(slot, i):
        at = slot * 96 + 16 * i + TOP
        return sums[pl.ds(at, SUB, stride=2), :] + sums[pl.ds(at + 1, SUB, stride=2), :]

    def restrict(at, blocks):
        @pl.loop(0, blocks)
        def _(b):
            column = at + RATIO * b
            for p in range(fine.pieces):
                found = stencil(fine, v, RATIO * column, p, BLOCK)
                defects = []
                for j, (here, total) in enumerate(found):
                    c = RATIO * column + j
                    change = get(fine, f, c, p) + get(fine, w, c, p) * total - 0.8 * here
                    defects.append(change * get(fine, iw, c, p))
                for slot in range(2):
                    sums[pl.ds(slot * 96 + p, SUB, stride=fine.pieces), :] = defects[2 * slot] + defects[2 * slot + 1]
            for slot in range(2):
                for i in range(4):
                    put_natural(
                        cf, column + slot, i, (paired(slot, i) * (1.0 / RATIO)) * natural(cw, column + slot, i)
                    )

    def correct(values, at, blocks):
        @pl.loop(0, blocks)
        def _(b):
            column = at + RATIO * b
            for slot in range(2):
                for i in range(-1, 5):
                    more = natural(values, column + slot, i)
                    place = slot * 96 + 16 * (i + 1)
                    sums[pl.ds(place, SUB, stride=2), :] = more
                    sums[pl.ds(place + 1, SUB, stride=2), :] = more
            for slot in range(2):
                for p in range(fine.pieces):
                    more = sums[pl.ds(slot * 96 + CTOP - TOP + p, SUB, stride=fine.pieces), :]
                    for j in range(RATIO):
                        c = fine.at(RATIO * (column + slot) + j, p)
                        v[pl.ds(c, SUB), :] = v[pl.ds(c, SUB), :] + more

    loaded(0)
    loaded(1)

    @pl.loop(0, fine.columns)
    def _(c):
        for p in range(fine.pieces):
            s, n = (1, 7) if p < 4 else (0, 8) if p == 4 else (0, 7)
            at = (c + fine.halo) * fine.width + p * SUB + s
            g4 = 4.0 + ra[pl.ds(at, n), :]
            weight = 0.8 / g4
            w[pl.ds(at, n), :] = weight
            f[pl.ds(at, n), :] = weight * rs[pl.ds(at, n), :]
            iw[pl.ds(at, n), :] = 1.25 * g4

    @pl.loop(0, coarse.columns // 2)
    def _(b):
        for slot in range(2):
            c = RATIO * (2 * b + slot)
            for p in range(fine.pieces):
                total = (4.0 + get(fine, ra, c, p)) + (4.0 + get(fine, ra, c + 1, p))
                sums[pl.ds(slot * 96 + p, SUB, stride=fine.pieces), :] = total
        for slot in range(2):
            for i in range(4):
                mean = paired(slot, i) * (1.0 / RATIO) - (4.0 * RATIO - 4.0)
                put_natural(cw, 2 * b + slot, i, 0.8 / mean)

    loaded(2)
    on_band = (band > 0).astype(jnp.int32) + (band < bands - 1).astype(jnp.int32)
    on_lane = (lane > 0).astype(jnp.int32) + (lane < lanes - 1).astype(jnp.int32)
    on_leg = sum((lane == source).astype(jnp.int32) for source, target in legs)
    pl.semaphore_wait(barrier, (on_band + 1) * (on_lane + 1) - 1 + on_leg)

    for name in ("u", "w", "f"):
        for q in sides:
            start(name, q)
    for name in ("u", "w", "f"):
        for q in corners:
            start(name, q)
    for name in ("u", "w", "f"):
        for q in rows_only:
            start(name, q)
    for q in sides + rows_only:
        start("cw", q)
    pass_on(("w", "f"))

    before = ((u, v), (v, x), (x, v))
    early_arrived(groups[0])
    for k, (old, new) in enumerate(before, 1):
        width = 4 * -(-(68 - 2 * k) // 4)
        sweep(fine, old, new, w, f, side(64 - k - width, k), width // 4)
    restrict(side(0, 2), 15)
    for q in sides:
        start("far", q)
    for q in sides + corners:
        start("near", q, jnp.logical_not(late(q)))
    for q in rows_only:
        start("far", q)
    late_arrived(groups[0])
    for k, (old, new) in enumerate(before, 1):
        sweep(fine, old, new, w, f, side(64 - k, k - 4), 1)
    restrict(side(30, 0), 1)
    for q in sides + corners:
        start("near", q, late(q))
    for q in rows_only:
        start("near", q)
    for q in sides + corners + rows_only:
        start("y", q)

    pass_on(("cw", "far", "y"))

    inner = []
    old = cf
    for k in range(2, INNER + 1):
        new = ca if k % 2 == 0 else cb
        inner.append((k, old, new))
        old = new
    sent(groups[0])
    for q in rows_only:
        arrived(groups[1], q)
    for q in sides:
        arrived(groups[1], q, jnp.logical_not(late(q)))
    for q in corners:
        start("turn", q, jnp.logical_not(late(q)))
    early_arrived(groups[3])
    for q in corners:
        arrived(groups[4], q, jnp.logical_not(late(q)))
    for k, old, new in inner:
        width = 4 * -(-(48 - 2 * k) // 4)
        sweep(coarse, old, new, cw, cf, side(33 - k - width, k - 1), width // 4)

    last = inner[-1][2]
    after = ((v, u), (u, v), (v, out))

    def take(outer, inner):
        @pl.loop(0, 2)
        def _(j):
            for p in range(fine.pieces):
                at = fine.at(outer + j, p)
                v[pl.ds(at, SUB), :] = y[pl.ds(at, SUB), :]

        for p, s in ((2, 0), (3, 0), (5, 7), (6, 7)):
            at = (inner + fine.halo) * fine.width + p * SUB + s
            v[pl.ds(at, 1), :] = y[pl.ds(at, 1), :]

    for q in sides:
        arrived(groups[1], q, late(q))
    for q in corners:
        start("turn", q, late(q))
    for names in groups[1:4]:
        sent(names)
    passed_on()
    early_arrived(groups[2])

    @pl.loop(0, fine.columns // SUB)
    def _(j):
        for p, s in ((1, 0), (2, 0), (6, 7), (7, 7)):
            at = (j * SUB + fine.halo) * fine.width + p * SUB + s
            v[pl.ds(at, SUB, stride=fine.width), :] = y[pl.ds(at, SUB, stride=fine.width), :]

    take(side(-3, 65), side(-1, 64))
    correct(last, side(-2, 12), 11)
    for m, (old, new) in enumerate(after, 1):
        width = 4 * -(-(43 - 2 * m) // 4)
        sweep(fine, old, new, w, f, side(40 - m - width, 24 + m), width // 4)

    late_arrived(groups[3])
    for q in corners:
        arrived(groups[4], q, late(q))
    sent(groups[4])
    for k, old, new in inner:
        sweep(coarse, old, new, cw, cf, side(33 - k, k - 17), 4)
    late_arrived(groups[2])
    take(side(65, -3), side(64, -1))
    correct(last, side(20, -2), 7)
    for m, (old, new) in enumerate(after, 1):
        sweep(fine, old, new, w, f, side(40 - m, m - 4), 7)


def per_device(source_terms, initial_values, absorption):
    rows, columns, cases = source_terms.shape
    fine = Grid(columns, (rows + 2 * TOP) // SUB, 8)
    coarse = Grid(columns // RATIO, (rows // RATIO + 2 * CTOP) // SUB, 18)

    def held(*shape):
        return pltpu.VMEM(shape + (cases,), jnp.float32)

    shapes = [held(fine.stored * fine.width) for _ in range(9)]
    shapes += [held(coarse.stored * coarse.width) for _ in range(4)]
    shapes += [held(2 * 96)]
    shapes += [held(22 * fine.width), held(16 * coarse.width)]
    shapes += [
        pltpu.SemaphoreType.DMA((3,)),
        pltpu.SemaphoreType.DMA((5 * len(DIRS),)),
        pltpu.SemaphoreType.DMA((5 * len(DIRS),)),
        pltpu.SemaphoreType.DMA((1,)),
        pltpu.SemaphoreType.DMA((5,)),
    ]
    pitched = pl.pallas_call(
        functools.partial(kernel, fine, coarse),
        out_shape=jax.ShapeDtypeStruct(((rows + 2 * TOP) * PITCH, cases), jnp.float32),
        in_specs=[pl.BlockSpec(memory_space=pltpu.HBM)] * 3,
        out_specs=pl.BlockSpec(memory_space=pltpu.VMEM),
        scratch_shapes=shapes,
        compiler_params=pltpu.CompilerParams(
            collective_id=0, has_side_effects=True, vmem_limit_bytes=52 * 1024 * 1024
        ),
    )(*[pltpu.with_memory_space_constraint(x, pltpu.HBM) for x in (source_terms, initial_values, absorption)])
    return pl.pallas_call(
        deliver,
        out_shape=jax.ShapeDtypeStruct(source_terms.shape, jnp.float32),
        in_specs=[pl.BlockSpec(memory_space=pltpu.VMEM)],
        out_specs=pl.BlockSpec(memory_space=pltpu.HBM),
        scratch_shapes=[pltpu.SemaphoreType.DMA],
    )(pitched)


def solution(mesh):
    placed = P(("shift", "band"), "lane", None)
    return jax.shard_map(
        per_device,
        mesh=mesh,
        in_specs=(placed, placed, placed),
        out_specs=placed,
        check_vma=False,
    )
```

```python
import functools

import jax
import jax.numpy as jnp
from jax import lax
from jax.experimental import pallas as pl
from jax.experimental.pallas import tpu as pltpu
from jax.sharding import PartitionSpec as P

RATIO = 2
INNER = 13
SUB = 8
BLOCK = 4
MESH = pl.DeviceIdType.MESH
DIRS = [(-1, 0), (1, 0), (0, -1), (0, 1), (-1, -1), (-1, 1), (1, -1), (1, 1)]
TOP = 4
CTOP = 16
LEVELS = 14
PITCH = 88
MARGIN = 8


class Grid:
    def __init__(self, columns, pieces, halo):
        self.columns, self.pieces, self.halo = columns, pieces, halo
        self.width = pieces * SUB
        self.stored = columns + 2 * halo

    def at(self, column, piece=0):
        return pl.multiple_of((column + self.halo) * self.width + piece * SUB, SUB)

    def boxes(self, ref):
        return ref.reshape(self.stored, self.pieces, SUB, 128)


def deliver(held, out_hbm, sem):
    rows, columns, _ = out_hbm.shape
    whole = held.reshape(rows + 2 * TOP, PITCH, 128).at[pl.ds(TOP, rows), pl.ds(MARGIN, columns), :]
    copy = pltpu.make_async_copy(whole, out_hbm, sem)
    copy.start()
    copy.wait()


def kernel(fine, coarse, src_hbm, init_hbm, abs_hbm, out, *scratch):
    u, v, x, w, f, y, iw, ra, rs, cw, cf, ca, cb, sums, fine_relay, coarse_relay, in_sem, send_sem, recv_sem, pass_sem, land_sem = scratch
    band, lane = lax.axis_index("band"), lax.axis_index("lane")
    bands, lanes = lax.axis_size("band"), lax.axis_size("lane")
    rows = fine.columns
    right = lane < lanes // 2

    def exists(q):
        dy, dx = q
        there = None
        if dy:
            there = (band > 0) if dy < 0 else (band < bands - 1)
        if dx:
            beside = (lane > 0) if dx < 0 else (lane < lanes - 1)
            there = beside if not dy else there & beside
        return there

    def name_of(q):
        return {"band": band + q[0], "lane": lane + q[1]}

    def late(q):
        return right if q[1] > 0 else jnp.logical_not(right)

    def side(if_right, if_left):
        return jnp.where(right, if_right, if_left)

    low, high = lanes // 2 - 1, lanes // 2
    ends = {(0, 1): (low, high), (0, -1): (high, low)}
    relays = {
        (0, 1): {1: lanes // 4 - 1, 2: 0, 3: lanes // 4},
        (0, -1): {1: lanes - lanes // 4, 2: lanes - 1, 3: lanes - lanes // 4 - 1},
    }
    legs = []
    for q, (source, target) in ends.items():
        for relay in relays[q].values():
            legs += [(source, relay), (relay, source), (relay, target), (target, relay)]

    barrier = pltpu.get_barrier_semaphore()
    for q in DIRS:
        @pl.when(exists(q))
        def _():
            pl.semaphore_signal(barrier, inc=1, device_id=name_of(q), device_id_type=MESH)
    for source, target in legs:
        @pl.when(lane == source)
        def _():
            pl.semaphore_signal(barrier, inc=1, device_id={"lane": target}, device_id_type=MESH)

    inputs = ((abs_hbm, ra), (src_hbm, rs), (init_hbm, u))
    for i, (ref, held) in enumerate(inputs):
        @pl.loop(0, rows)
        def _(row):
            at = row + TOP
            place = (at % fine.pieces) * SUB + at // fine.pieces
            to = held.reshape(fine.stored, fine.width, 128).at[
                pl.ds(fine.halo, fine.columns), pl.ds(place, 1), :
            ]
            pltpu.make_async_copy(ref.at[row].reshape(fine.columns, 1, 128), to, in_sem.at[i]).start()

    def loaded(i):
        ref, held = inputs[i]
        whole = held.reshape(fine.stored, fine.width, 128).at[pl.ds(fine.halo, fine.columns), pl.ds(0, rows), :]
        pltpu.make_async_copy(ref, whole, in_sem.at[i]).wait()

    zero = jnp.zeros((SUB, 128), jnp.float32)
    for dx in (-1, 1):
        @pl.when(jnp.logical_not(exists((0, dx))))
        def _():
            for g, refs, depth in ((fine, (u, w, f, y), 4), (coarse, (cw, cf), LEVELS)):
                @pl.loop(0, depth)
                def _(j):
                    column = j - depth if dx < 0 else g.columns + j
                    for ref in refs:
                        for p in range(g.pieces):
                            ref[pl.ds(g.at(column, p), SUB), :] = zero

    for dy in (-1, 1):
        @pl.when(jnp.logical_not(exists((dy, 0))))
        def _():
            @pl.loop(0, fine.stored // SUB)
            def _(j):
                for ref in (u, w, f, y):
                    for p in range(TOP):
                        place = p * SUB if dy < 0 else (fine.pieces - 1 - p) * SUB + SUB - 1
                        ref[pl.ds(j * SUB * fine.width + place, SUB, stride=fine.width), :] = zero

            @pl.loop(0, coarse.stored)
            def _(j):
                for ref in (cw, cf):
                    for p in range(coarse.pieces):
                        at = coarse.width * j + p * SUB + (0 if dy < 0 else SUB - 2)
                        ref[pl.ds(at, 2), :] = zero[:2]

    def columns_of(g, dx, depth, skip=0):
        if dx > 0:
            return g.halo + g.columns - depth - skip, g.halo - depth - skip, depth
        return g.halo + skip, g.halo + g.columns + skip, depth

    def outside(g, dx, depth, skip):
        return g.halo + g.columns + skip if dx > 0 else g.halo - depth - skip

    def fine_rows(dy, depth, skip=0):
        if dy > 0:
            return [((5 - depth - skip, 7), (4 - depth - skip, 0), (depth, 1))]
        return [((4 + skip, 0), (5 + skip, 7), (depth, 1))]

    def coarse_rows(dy, depth):
        e = depth - SUB
        if e <= 0:
            if dy > 0:
                return [((SUB - depth, 5), (SUB - depth, 1), (depth, 1))]
            return [((0, 2), (0, 6), (depth, 1))]
        if dy > 0:
            return [((SUB - e, 4), (SUB - e, 0), (e, 2)), ((0, 5), (0, 1), (SUB - e, 1))]
        return [((0, 2), (0, 6), (e, 2)), ((e, 2), (e, 6), (SUB - e, 1))]

    own = [((0, 1), (0, 1), (4, 7)), ((4, 0), (4, 0), (1, 8)), ((5, 0), (5, 0), (4, 7))]
    middle = [((0, 2), (0, 2), (SUB, 4))]

    copies, used, volume = {}, {}, {}
    offsets = {"w": 0, "f": 9, "y": 18, "cw": 0, "far": 8}

    def add(name, g, source, target, q, columns, places, paths=(0,)):
        from_column, to_column, count = columns
        for i, ((p, s), (pt, st), (np_, ns)) in enumerate(places):
            here = g.boxes(source).at[pl.ds(from_column, count), pl.ds(p, np_), pl.ds(s, ns), :]
            there = g.boxes(target).at[pl.ds(to_column, count), pl.ds(pt, np_), pl.ds(st, ns), :]
            path = paths[i % len(paths)]
            relay = None
            if path:
                held = fine_relay if g is fine else coarse_relay
                base = used.setdefault((name, q, path), 0)
                used[name, q, path] = base + count
                base += offsets[name]
                relay = held.reshape(held.shape[0] // g.width, g.pieces, SUB, 128).at[
                    pl.ds(base, count), pl.ds(p, np_), pl.ds(s, ns), :
                ]
            copies.setdefault((name, q), []).append((here, there, path, relay))
            volume[name, q, path] = volume.get((name, q, path), 0) + count * np_ * ns

    for q in DIRS:
        dy, dx = q
        for name, source, target, depth, corner in (("u", u, u, 4, 3), ("w", w, w, 3, 2), ("f", f, f, 3, 2)):
            if not dy and name == "u":
                add(name, fine, source, target, q, columns_of(fine, dx, depth), own)
            elif not dy:
                add(name, fine, source, target, q, columns_of(fine, dx, 3), own, (2 if name == "w" else 2,))
            elif not dx:
                add(name, fine, source, target, q, (fine.halo, fine.halo, fine.columns), fine_rows(dy, depth))
            else:
                add(name, fine, source, target, q, columns_of(fine, dx, corner), fine_rows(dy, corner))
        if not dy:
            add("y", fine, v, y, q, columns_of(fine, dx, 2, 1), own, (2, 0, 2))
        elif not dx:
            add("y", fine, v, y, q, (fine.halo, fine.halo, fine.columns), fine_rows(dy, 2, 1))
        else:
            add("y", fine, v, y, q, columns_of(fine, dx, 2), fine_rows(dy, 2))

    for q in DIRS:
        dy, dx = q
        if not dy:
            add("near", coarse, cf, cf, q, columns_of(coarse, dx, 2), middle)
            for path, count, skip in ((0, 4, 0), (1, 3, 4), (2, 3, 7), (3, 3, 10)):
                add("cw", coarse, cw, cw, q, columns_of(coarse, dx, count, skip), middle, (path,))
            for path, count, skip in ((0, 3, 2), (1, 3, 5), (2, 3, 8), (3, 3, 11)):
                add("far", coarse, cf, cf, q, columns_of(coarse, dx, count, skip), middle, (path,))
        elif not dx:
            place = coarse_rows(dy, LEVELS - 1)
            add("cw", coarse, cw, cw, q, (coarse.halo, coarse.halo, coarse.columns), place)
            place = coarse_rows(dy, LEVELS)
            at = coarse.halo + side(coarse.columns - 2, 0)
            add("near", coarse, cf, cf, q, (at, at, 2), place)
            at = coarse.halo + side(0, 2)
            add("far", coarse, cf, cf, q, (at, at, coarse.columns - 2), place)
        else:
            add("near", coarse, cf, cf, q, columns_of(coarse, dx, 2), coarse_rows(dy, LEVELS - 1))
            for count, skip, depth in ((2, 0, 12), (3, 2, 10), (4, 5, 7), (3, 9, 3)):
                at = outside(coarse, dx, count, skip)
                add("turn", coarse, cw, cw, q, (at, at, count), coarse_rows(dy, depth))
            for count, skip, depth in ((3, 2, 11), (4, 5, 8), (4, 9, 4)):
                at = outside(coarse, dx, count, skip)
                add("turn", coarse, cf, cf, q, (at, at, count), coarse_rows(dy, depth))

    groups = (("u", "w", "f"), ("cw", "far"), ("y",), ("near",), ("turn",))
    relayed = ("w", "f", "cw", "far", "y")

    def place_of(name, q):
        group = [name in names for names in groups].index(True)
        return group * len(DIRS) + DIRS.index(q)

    def from_side(name, q):
        return (-q[0], q[1]) if name == "turn" else (-q[0], -q[1])

    def wait(sem, count):
        if not count:
            return
        rows_of = u.at[pl.ds(0, count), :]
        pltpu.make_async_copy(rows_of, rows_of, sem).wait()

    def total(names, q, path=None):
        return sum(n for (name, d, way), n in volume.items() if name in names and d == q and path in (None, way))

    def copies_of(name, q):
        for here, there, path, relay in copies[name, q]:
            yield path, pltpu.make_async_remote_copy(
                src_ref=here,
                dst_ref=there,
                send_sem=send_sem.at[place_of(name, q)],
                recv_sem=recv_sem.at[place_of(name, from_side(name, q))],
                device_id=name_of((q[0], 0) if name == "turn" else q),
                device_id_type=MESH,
            )

    def legs_of(name, q, way=None):
        back = (-q[0], -q[1])
        for here, there, path, relay in copies[name, q]:
            if path and way in (None, path):
                yield pltpu.make_async_remote_copy(
                    src_ref=here,
                    dst_ref=relay,
                    send_sem=send_sem.at[place_of(name, q)],
                    recv_sem=land_sem.at[relayed.index(name)],
                    device_id={"lane": relays[q][path]},
                    device_id_type=MESH,
                ), pltpu.make_async_remote_copy(
                    src_ref=relay,
                    dst_ref=there,
                    send_sem=pass_sem.at[0],
                    recv_sem=recv_sem.at[place_of(name, back)],
                    device_id={"lane": ends[q][1]},
                    device_id_type=MESH,
                )

    def start(name, q, when=None):
        ready = exists(q) if when is None else exists(q) & when
        direct = ready
        if any(path for *_, path, relay in copies[name, q]):
            direct = ready & (lane != ends[q][0])

            @pl.when(ready & (lane == ends[q][0]))
            def _():
                for there, on in legs_of(name, q):
                    there.start()
                for path, copy in copies_of(name, q):
                    if not path:
                        copy.start()

        @pl.when(direct)
        def _():
            for path, copy in copies_of(name, q):
                copy.start()

    def pass_on(names):
        for q in ends:
            for way, relay_lane in relays[q].items():
                @pl.when(lane == relay_lane)
                def _():
                    for name in names:
                        if total((name,), q, way):
                            wait(land_sem.at[relayed.index(name)], total((name,), q, way))
                            for there, on in legs_of(name, q, way):
                                on.start()

    def passed_on():
        for q in ends:
            for way, relay_lane in relays[q].items():
                @pl.when(lane == relay_lane)
                def _():
                    wait(pass_sem.at[0], total(relayed, q, way))

    def sent(names):
        for q in DIRS:
            @pl.when(exists(q))
            def _():
                wait(send_sem.at[place_of(names[0], q)], total(names, q))

    def arrived(names, q, when=None):
        @pl.when(exists(q) if when is None else exists(q) & when)
        def _():
            wait(recv_sem.at[place_of(names[0], q)], total(names, from_side(names[0], q)))

    rows_only, sides, corners = DIRS[:2], DIRS[2:4], DIRS[4:]

    def early_arrived(names):
        for q in rows_only:
            arrived(names, q)
        for q in sides + corners:
            arrived(names, q, jnp.logical_not(late(q)))

    def late_arrived(names):
        for q in sides + corners:
            arrived(names, q, late(q))

    def get(g, ref, column, p):
        return ref[pl.ds(g.at(column, p), SUB), :]

    def stencil(g, old, column, p, count):
        here = [get(g, old, column + j, p) for j in range(-1, count + 1)]
        found = []
        for j in range(count):
            up = get(g, old, column + j, p - 1) if p else pltpu.roll(get(g, old, column + j, g.pieces - 1), 1, 0)
            if p < g.pieces - 1:
                down = get(g, old, column + j, p + 1)
            else:
                down = pltpu.roll(get(g, old, column + j, 0), SUB - 1, 0)
            found.append((here[j + 1], (up + down) + (here[j] + here[j + 2])))
        return found

    def sweep(g, old, new, weight, load, at, blocks):
        @pl.loop(0, blocks, unroll=2 if blocks % 2 == 0 else 1)
        def _(b):
            column = at + BLOCK * b
            for p in range(g.pieces):
                for j, (here, total) in enumerate(stencil(g, old, column, p, BLOCK)):
                    c = column + j
                    value = 0.2 * here + get(g, load, c, p) + get(g, weight, c, p) * total
                    if new is out:
                        new[pl.ds(p * PITCH + c + MARGIN, SUB, stride=g.pieces * PITCH), :] = value
                    else:
                        new[pl.ds(g.at(c, p), SUB), :] = value

    def natural(ref, column, i):
        return ref[pl.ds((column + coarse.halo) * coarse.width + 2 + i, SUB, stride=coarse.pieces), :]

    def put_natural(ref, column, i, value):
        ref[pl.ds((column + coarse.halo) * coarse.width + 2 + i, SUB, stride=coarse.pieces), :] = value

    def paired(slot, i):
        at = slot * 96 + 16 * i + TOP
        return sums[pl.ds(at, SUB, stride=2), :] + sums[pl.ds(at + 1, SUB, stride=2), :]

    def restrict(at, blocks):
        @pl.loop(0, blocks)
        def _(b):
            column = at + RATIO * b
            for p in range(fine.pieces):
                found = stencil(fine, v, RATIO * column, p, BLOCK)
                defects = []
                for j, (here, total) in enumerate(found):
                    c = RATIO * column + j
                    change = get(fine, f, c, p) + get(fine, w, c, p) * total - 0.8 * here
                    defects.append(change * get(fine, iw, c, p))
                for slot in range(2):
                    sums[pl.ds(slot * 96 + p, SUB, stride=fine.pieces), :] = defects[2 * slot] + defects[2 * slot + 1]
            for slot in range(2):
                for i in range(4):
                    put_natural(
                        cf, column + slot, i, (paired(slot, i) * (1.0 / RATIO)) * natural(cw, column + slot, i)
                    )

    def correct(values, at, blocks):
        @pl.loop(0, blocks)
        def _(b):
            column = at + RATIO * b
            for slot in range(2):
                for i in range(-1, 5):
                    more = natural(values, column + slot, i)
                    place = slot * 96 + 16 * (i + 1)
                    sums[pl.ds(place, SUB, stride=2), :] = more
                    sums[pl.ds(place + 1, SUB, stride=2), :] = more
            for slot in range(2):
                for p in range(fine.pieces):
                    more = sums[pl.ds(slot * 96 + CTOP - TOP + p, SUB, stride=fine.pieces), :]
                    for j in range(RATIO):
                        c = fine.at(RATIO * (column + slot) + j, p)
                        v[pl.ds(c, SUB), :] = v[pl.ds(c, SUB), :] + more

    loaded(0)
    loaded(1)

    @pl.loop(0, fine.columns)
    def _(c):
        for p in range(fine.pieces):
            s, n = (1, 7) if p < 4 else (0, 8) if p == 4 else (0, 7)
            at = (c + fine.halo) * fine.width + p * SUB + s
            g4 = 4.0 + ra[pl.ds(at, n), :]
            weight = 0.8 / g4
            w[pl.ds(at, n), :] = weight
            f[pl.ds(at, n), :] = weight * rs[pl.ds(at, n), :]
            iw[pl.ds(at, n), :] = 1.25 * g4

    @pl.loop(0, coarse.columns // 2)
    def _(b):
        for slot in range(2):
            c = RATIO * (2 * b + slot)
            for p in range(fine.pieces):
                total = (4.0 + get(fine, ra, c, p)) + (4.0 + get(fine, ra, c + 1, p))
                sums[pl.ds(slot * 96 + p, SUB, stride=fine.pieces), :] = total
        for slot in range(2):
            for i in range(4):
                mean = paired(slot, i) * (1.0 / RATIO) - (4.0 * RATIO - 4.0)
                put_natural(cw, 2 * b + slot, i, 0.8 / mean)

    loaded(2)
    on_band = (band > 0).astype(jnp.int32) + (band < bands - 1).astype(jnp.int32)
    on_lane = (lane > 0).astype(jnp.int32) + (lane < lanes - 1).astype(jnp.int32)
    on_leg = sum((lane == source).astype(jnp.int32) for source, target in legs)
    pl.semaphore_wait(barrier, (on_band + 1) * (on_lane + 1) - 1 + on_leg)

    for name in ("u", "w", "f"):
        for q in sides:
            start(name, q)
    for name in ("u", "w", "f"):
        for q in corners:
            start(name, q)
    for name in ("u", "w", "f"):
        for q in rows_only:
            start(name, q)
    for q in sides + rows_only:
        start("cw", q)
    pass_on(("w", "f"))

    before = ((u, v), (v, x), (x, v))
    early_arrived(groups[0])
    for k, (old, new) in enumerate(before, 1):
        width = 4 * -(-(68 - 2 * k) // 4)
        sweep(fine, old, new, w, f, side(64 - k - width, k), width // 4)
    restrict(side(0, 2), 15)
    for q in sides:
        start("far", q)
    for q in sides + corners:
        start("near", q, jnp.logical_not(late(q)))
    for q in rows_only:
        start("far", q)
    late_arrived(groups[0])
    for k, (old, new) in enumerate(before, 1):
        sweep(fine, old, new, w, f, side(64 - k, k - 4), 1)
    restrict(side(30, 0), 1)
    for q in sides + corners:
        start("near", q, late(q))
    for q in rows_only:
        start("near", q)
    for q in sides + corners + rows_only:
        start("y", q)

    pass_on(("cw", "far", "y"))

    inner = []
    old = cf
    for k in range(2, INNER + 1):
        new = ca if k % 2 == 0 else cb
        inner.append((k, old, new))
        old = new
    sent(groups[0])
    for q in rows_only:
        arrived(groups[1], q)
    for q in sides:
        arrived(groups[1], q, jnp.logical_not(late(q)))
    for q in corners:
        start("turn", q, jnp.logical_not(late(q)))
    early_arrived(groups[3])
    for q in corners:
        arrived(groups[4], q, jnp.logical_not(late(q)))
    for k, old, new in inner:
        width = 4 * -(-(48 - 2 * k) // 4)
        sweep(coarse, old, new, cw, cf, side(33 - k - width, k - 1), width // 4)

    last = inner[-1][2]
    after = ((v, u), (u, v), (v, out))

    def take(outer, inner):
        @pl.loop(0, 2)
        def _(j):
            for p in range(fine.pieces):
                at = fine.at(outer + j, p)
                v[pl.ds(at, SUB), :] = y[pl.ds(at, SUB), :]

        for p, s in ((2, 0), (3, 0), (5, 7), (6, 7)):
            at = (inner + fine.halo) * fine.width + p * SUB + s
            v[pl.ds(at, 1), :] = y[pl.ds(at, 1), :]

    for q in sides:
        arrived(groups[1], q, late(q))
    for q in corners:
        start("turn", q, late(q))
    for names in groups[1:4]:
        sent(names)
    passed_on()
    early_arrived(groups[2])

    @pl.loop(0, fine.columns // SUB)
    def _(j):
        for p, s in ((1, 0), (2, 0), (6, 7), (7, 7)):
            at = (j * SUB + fine.halo) * fine.width + p * SUB + s
            v[pl.ds(at, SUB, stride=fine.width), :] = y[pl.ds(at, SUB, stride=fine.width), :]

    take(side(-3, 65), side(-1, 64))
    correct(last, side(-2, 12), 11)
    for m, (old, new) in enumerate(after, 1):
        width = 4 * -(-(43 - 2 * m) // 4)
        sweep(fine, old, new, w, f, side(40 - m - width, 24 + m), width // 4)

    late_arrived(groups[3])
    for q in corners:
        arrived(groups[4], q, late(q))
    sent(groups[4])
    for k, old, new in inner:
        sweep(coarse, old, new, cw, cf, side(33 - k, k - 17), 4)
    late_arrived(groups[2])
    take(side(65, -3), side(64, -1))
    correct(last, side(20, -2), 7)
    for m, (old, new) in enumerate(after, 1):
        sweep(fine, old, new, w, f, side(40 - m, m - 4), 7)


def per_device(source_terms, initial_values, absorption):
    rows, columns, cases = source_terms.shape
    fine = Grid(columns, (rows + 2 * TOP) // SUB, 8)
    coarse = Grid(columns // RATIO, (rows // RATIO + 2 * CTOP) // SUB, 18)

    def held(*shape):
        return pltpu.VMEM(shape + (cases,), jnp.float32)

    shapes = [held(fine.stored * fine.width) for _ in range(9)]
    shapes += [held(coarse.stored * coarse.width) for _ in range(4)]
    shapes += [held(2 * 96)]
    shapes += [held(22 * fine.width), held(16 * coarse.width)]
    shapes += [
        pltpu.SemaphoreType.DMA((3,)),
        pltpu.SemaphoreType.DMA((5 * len(DIRS),)),
        pltpu.SemaphoreType.DMA((5 * len(DIRS),)),
        pltpu.SemaphoreType.DMA((1,)),
        pltpu.SemaphoreType.DMA((5,)),
    ]
    pitched = pl.pallas_call(
        functools.partial(kernel, fine, coarse),
        out_shape=jax.ShapeDtypeStruct(((rows + 2 * TOP) * PITCH, cases), jnp.float32),
        in_specs=[pl.BlockSpec(memory_space=pltpu.HBM)] * 3,
        out_specs=pl.BlockSpec(memory_space=pltpu.VMEM),
        scratch_shapes=shapes,
        compiler_params=pltpu.CompilerParams(
            collective_id=0, has_side_effects=True, vmem_limit_bytes=52 * 1024 * 1024
        ),
    )(*[pltpu.with_memory_space_constraint(x, pltpu.HBM) for x in (source_terms, initial_values, absorption)])
    return pl.pallas_call(
        deliver,
        out_shape=jax.ShapeDtypeStruct(source_terms.shape, jnp.float32),
        in_specs=[pl.BlockSpec(memory_space=pltpu.VMEM)],
        out_specs=pl.BlockSpec(memory_space=pltpu.HBM),
        scratch_shapes=[pltpu.SemaphoreType.DMA],
    )(pitched)


def solution(mesh):
    placed = P(("shift", "band"), "lane", None)
    return jax.shard_map(
        per_device,
        mesh=mesh,
        in_specs=(placed, placed, placed),
        out_specs=placed,
        check_vma=False,
    )
```
